32 devices in a mesh: gx: 2 (over y), gy: 4 (over z), gz: 4 (over x, core).
Axes of the slice: x: 2, y: 2, z: 4, core: 2. Of those that a mesh axis runs over, the one named last changes fastest.
Arguments:
- kinematics: float32 [18, 8192], P(None, ('gx', 'gy', 'gz')), may hold values from -6 to 6
- pair_offsets: float32 [3, 16, 8192], P(None, None, ('gx', 'gy', 'gz')), may hold values from -1 to 1
- pair_index: int32 [16, 8192], P(None, ('gx', 'gy', 'gz')), may hold values from 0 to 687, as said below
- neighbour_count: int32 [8192], P(('gx', 'gy', 'gz')), may hold values from 1 to 16
- send_rows: int32 [27, 512], P(None, ('gx', 'gy', 'gz')), may hold values from 0 to 255
- migrate_dir: int32 [8192], P(('gx', 'gy', 'gz')), may hold values from 0 to 26, as said below
- migrate_slot: int32 [8192], P(('gx', 'gy', 'gz')), may hold values from 0 to 3, as said below
- enc_node_w1: float32 [15, 128], replicated, may hold values from -1.5 to 1.5
- enc_node_w2: bfloat16 [128, 128], replicated, may hold values from -0.5 to 0.5
- enc_edge_w1: float32 [4, 128], replicated, may hold values from -3 to 3
- enc_edge_w2: bfloat16 [128, 128], replicated, may hold values from -0.5 to 0.5
- edge_w1: bfloat16 [3, 384, 128], replicated, may hold values from -0.3125 to 0.3125
- edge_w2: bfloat16 [3, 128, 128], replicated, may hold values from -0.5 to 0.5
- node_w1: bfloat16 [3, 256, 128], replicated, may hold values from -0.375 to 0.375
- node_w2: bfloat16 [3, 128, 128], replicated, may hold values from -0.5 to 0.5
- edge_gain: float32 [3, 128], replicated, may hold values from 0.25 to 1.75
- node_gain: float32 [3, 128], replicated, may hold values from 0.25 to 1.75
- dec_w1: bfloat16 [128, 128], replicated, may hold values from -0.5 to 0.5
- dec_w2: float32 [3, 128], replicated, may hold values from -0.5 to 0.5
Outputs:
- stayed: float32 [18, 8192], P(None, ('gx', 'gy', 'gz'))
- arrived: float32 [18, 3456], P(None, ('gx', 'gy', 'gz'))
The draws below stay inside these ranges and needn't reach their ends.
Inputs may be any that keep to these rules, and one draw needn't show every extreme that they name: `pair_index`: A value below 256 names a row of the particle's own subdomain. A value v of 256 or more names ghost row v - 256; its direction (v - 256) // 16 is never 13 and points to a subdomain inside the grid. How many ghost rows of a direction are named differs between directions and subdomains. `migrate_dir`: A value other than 13 points to a subdomain inside the grid. On one subdomain at most 4 particles share a direction, and on every subdomain some direction has exactly 4. `migrate_slot`: among the particles of one subdomain that leave in one direction the slots are distinct; for staying particles the slot means nothing.
All inputs are finite; a program needn't handle non-finite values.
Results may differ from the reference program's by a relative error of at most 0.0085.
Values may be sent and summed in bfloat16 or wider, within the bound.
A program may use at most 64 MiB of HBM per device.

```python
import jax
import jax.numpy as jnp
import numpy as np
from jax import lax

LATENT = 128
HIDDEN_SIZE = 128
PART_DEV = 256
K = 16
GHOST = 16
MIG = 4
ROUNDS = 3
STATE = 18
PARTICLES = 8192
SENDS = 512
N_GX = 2
N_GY = 4
N_GZ = 4


def inside_table():
    device_total = N_GX * N_GY * N_GZ
    direction = np.arange(27)
    shifts = np.stack([direction // 9 - 1, direction // 3 % 3 - 1, direction % 3 - 1], axis=1)
    device = jnp.arange(device_total, dtype=jnp.int32)[:, None]
    along_first = device // (N_GY * N_GZ) + jnp.asarray(shifts[:, 0], jnp.int32)[None, :]
    along_second = device // N_GZ % N_GY + jnp.asarray(shifts[:, 1], jnp.int32)[None, :]
    along_third = device % N_GZ + jnp.asarray(shifts[:, 2], jnp.int32)[None, :]
    inside = (along_first >= 0) & (along_first < N_GX) & (along_second >= 0) & (along_second < N_GY) & (along_third >= 0) & (along_third < N_GZ)
    inside = inside & jnp.asarray(direction != 13)[None, :]
    kind_table = jnp.asarray(np.abs(shifts).sum(axis=1), jnp.int32)
    return (inside, kind_table)


def valid_order(inside):
    ranking = jnp.where(inside, 0, 1) * 32 + jnp.arange(27, dtype=jnp.int32)[None, :]
    ordered = jnp.argsort(ranking, axis=1).astype(jnp.int32)
    return (ordered, jnp.sum(inside.astype(jnp.int32), axis=1))


def draw_pair_index(key, part):
    device_total = N_GX * N_GY * N_GZ
    inside, kind_table = inside_table()
    ordered, valid_total = valid_order(inside)
    subkeys = jax.random.split(jax.random.fold_in(key, 11), 8)
    face_fill = jax.random.randint(subkeys[0], (device_total, 27), 3 * GHOST // 4, GHOST + 1)
    edge_fill = jax.random.randint(subkeys[1], (device_total, 27), GHOST // 2, GHOST + 1)
    corner_fill = jax.random.randint(subkeys[2], (device_total, 27), GHOST // 2, GHOST + 1)
    filled = jnp.where(kind_table[None, :] == 1, face_fill, jnp.where(kind_table[None, :] == 2, edge_fill, corner_fill))
    heavy_pick = jax.random.randint(subkeys[3], (device_total,), 0, valid_total)
    heavy_dir = jnp.take_along_axis(ordered, heavy_pick[:, None], axis=1)
    filled = jnp.where(jnp.arange(27, dtype=jnp.int32)[None, :] == heavy_dir, GHOST, filled)
    draw_shape = (K, device_total, PART_DEV)
    ghostly = jax.random.randint(subkeys[4], draw_shape, 0, 10) < 3
    local_row = jax.random.randint(subkeys[5], draw_shape, 0, PART_DEV)
    device = jnp.arange(device_total, dtype=jnp.int32)[None, :, None]
    picked_rank = jax.random.randint(subkeys[6], draw_shape, 0, valid_total[None, :, None])
    direction = ordered[device, picked_rank]
    slot_index = jax.random.randint(subkeys[7], draw_shape, 0, filled[device, direction])
    entries = jnp.where(ghostly, PART_DEV + direction * GHOST + slot_index, local_row)
    return entries.reshape(K, device_total * PART_DEV).astype(jnp.int32)


def migration_plan(key):
    device_total = N_GX * N_GY * N_GZ
    inside, kind_table = inside_table()
    ordered, valid_total = valid_order(inside)
    subkeys = jax.random.split(jax.random.fold_in(key, 23), 4)
    taken = jax.random.randint(subkeys[0], (device_total, 27), 0, MIG + 1)
    taken = jnp.where(inside, taken, 0)
    heavy_pick = jax.random.randint(subkeys[1], (device_total,), 0, valid_total)
    heavy_dir = jnp.take_along_axis(ordered, heavy_pick[:, None], axis=1)
    taken = jnp.where(jnp.arange(27, dtype=jnp.int32)[None, :] == heavy_dir, MIG, taken)
    permuted = jax.vmap(lambda subkey: jax.random.permutation(subkey, PART_DEV))(jax.random.split(subkeys[2], device_total))
    ranks = jnp.argsort(permuted, axis=1).astype(jnp.int32)
    direction = jnp.minimum(ranks // MIG, 26)
    slot_index = ranks % MIG
    device = jnp.arange(device_total, dtype=jnp.int32)[:, None]
    leaving = (ranks < 27 * MIG) & (slot_index < taken[device, direction])
    spare = jax.random.randint(subkeys[3], (device_total, PART_DEV), 0, MIG)
    targets = jnp.where(leaving, direction, 13)
    slots_out = jnp.where(leaving, slot_index, spare)
    return (targets.reshape(-1).astype(jnp.int32), slots_out.reshape(-1).astype(jnp.int32))


def draw_migrate_dir(key, part):
    return migration_plan(key)[0]


def draw_migrate_slot(key, part):
    return migration_plan(key)[1]


def plant(array, rng, low, top_value):
    spot = [jax.random.randint(jax.random.fold_in(rng, axis), (), 0, length) for axis, length in enumerate(array.shape)]
    main_axis = array.shape.index(max(array.shape))
    next_to = spot[:main_axis] + [(spot[main_axis] + 1) % array.shape[main_axis]] + spot[main_axis + 1:]
    return array.at[tuple(spot)].set(low).at[tuple(next_to)].set(top_value)


def level_of(key, extent, cuts, smallest, top_value):
    gain = 1.0
    for axis_at, blocks in cuts:
        draws = jax.random.uniform(jax.random.fold_in(jax.random.fold_in(key, 6), axis_at), (blocks,), jnp.float32, smallest / len(cuts), top_value / len(cuts))
        gain = gain * jnp.repeat(jnp.exp(draws), extent[axis_at] // blocks).reshape((-1,) + (1,) * (len(extent) - 1 - axis_at))
    return gain


def centred(stream_key, shape, deviation, reach, cuts=(), held_as=jnp.bfloat16):
    array = deviation * jax.random.normal(stream_key, shape, jnp.float32)
    if cuts:
        array = array * level_of(stream_key, shape, cuts, -0.22, 0.18)
    return jnp.clip(array, -reach, reach).astype(held_as)


def setup_inputs(seed: int = 0) -> dict:
    keys = jax.random.split(jax.random.key(seed), 20)
    return {
        "kinematics": centred(keys[0], (STATE, PARTICLES), 1.0, 6.0, ((1, 32),), jnp.float32),
        "pair_offsets": jnp.clip(jax.random.uniform(keys[1], (3, K, PARTICLES), jnp.float32, -1.0, 1.0) * level_of(keys[1], (3, K, PARTICLES), ((2, 32),), -0.4, 0.0), -1.0, 1.0),
        "pair_index": draw_pair_index(jax.random.fold_in(keys[19], 71), 0),
        "neighbour_count": plant(jax.random.randint(keys[3], (PARTICLES,), 1, K + 1), jax.random.fold_in(keys[3], 1), 1, K).astype(jnp.int32),
        "send_rows": plant(jax.random.randint(keys[4], (27, SENDS), 0, PART_DEV), jax.random.fold_in(keys[4], 1), 0, PART_DEV - 1).astype(jnp.int32),
        "migrate_dir": draw_migrate_dir(jax.random.fold_in(keys[19], 71), 0),
        "migrate_slot": draw_migrate_slot(jax.random.fold_in(keys[19], 71), 0),
        "enc_node_w1": centred(keys[7], (STATE - 3, HIDDEN_SIZE), (STATE - 3) ** -0.5, 1.5, (), jnp.float32),
        "enc_node_w2": centred(keys[8], (HIDDEN_SIZE, LATENT), HIDDEN_SIZE ** -0.5, 0.5),
        "enc_edge_w1": centred(keys[9], (4, HIDDEN_SIZE), 4 ** -0.5, 3.0, (), jnp.float32),
        "enc_edge_w2": centred(keys[10], (HIDDEN_SIZE, LATENT), HIDDEN_SIZE ** -0.5, 0.5),
        "edge_w1": centred(keys[11], (ROUNDS, 3 * LATENT, HIDDEN_SIZE), (3 * LATENT) ** -0.5, 0.3125),
        "edge_w2": centred(keys[12], (ROUNDS, HIDDEN_SIZE, LATENT), HIDDEN_SIZE ** -0.5, 0.5),
        "node_w1": centred(keys[13], (ROUNDS, 2 * LATENT, HIDDEN_SIZE), (2 * LATENT) ** -0.5, 0.375),
        "node_w2": centred(keys[14], (ROUNDS, HIDDEN_SIZE, LATENT), HIDDEN_SIZE ** -0.5, 0.5),
        "edge_gain": jnp.clip(1.0 + 0.15 * jax.random.normal(keys[15], (ROUNDS, LATENT), jnp.float32), 0.25, 1.75),
        "node_gain": jnp.clip(1.0 + 0.15 * jax.random.normal(keys[16], (ROUNDS, LATENT), jnp.float32), 0.25, 1.75),
        "dec_w1": centred(keys[17], (LATENT, HIDDEN_SIZE), LATENT ** -0.5, 0.5),
        "dec_w2": centred(keys[18], (3, HIDDEN_SIZE), HIDDEN_SIZE ** -0.5, 0.5, (), jnp.float32),
    }


norm_eps = 1e-05

def layer_norm(values):
    center = values - lax.optimization_barrier(jnp.mean(values, axis=-1, keepdims=True))
    spread = lax.optimization_barrier(jnp.mean(center * center, axis=-1, keepdims=True))
    return center * lax.rsqrt(spread + norm_eps)

def encode_edges(offsets, first_weight, second_weight):
    squared = lax.optimization_barrier(jnp.sum(offsets * offsets, axis=0, keepdims=True))
    features = jnp.concatenate([offsets, squared], axis=0)
    hidden = jnp.maximum(jnp.einsum('ckp,ch->kph', features, first_weight, precision=lax.Precision.HIGHEST), 0.0).astype(jnp.bfloat16)
    pair_slots, particles, inner_width = hidden.shape
    result = jnp.dot(hidden.reshape(pair_slots * particles, inner_width), second_weight, preferred_element_type=jnp.float32)
    return layer_norm(result).astype(jnp.bfloat16).reshape(pair_slots, particles, second_weight.shape[1])

def message_round(latent, extended, edge_latent, pair_index, neighbour_count, edge_first, edge_second, node_first, node_second, edge_scale, node_scale, block_pairs):
    latent_width = latent.shape[1]
    pair_slots, particles = pair_index.shape
    sender_proj = jnp.dot(extended, edge_first[2 * latent_width:], preferred_element_type=jnp.float32)
    receiver_proj = jnp.dot(latent, edge_first[latent_width:2 * latent_width], preferred_element_type=jnp.float32)
    summed = jnp.zeros((particles, edge_second.shape[1]), jnp.float32)
    for first_pair in range(0, pair_slots, block_pairs):
        chosen = pair_index[first_pair:first_pair + block_pairs]
        edge_rows = edge_latent[first_pair:first_pair + block_pairs].reshape(block_pairs * particles, latent_width)
        pre_act = jnp.dot(edge_rows, edge_first[:latent_width], preferred_element_type=jnp.float32).reshape(block_pairs, particles, -1)
        pre_act = pre_act + receiver_proj[None] + sender_proj[chosen]
        hidden = jnp.maximum(pre_act, 0.0).astype(jnp.bfloat16)
        message = layer_norm(jnp.dot(hidden.reshape(block_pairs * particles, -1), edge_second, preferred_element_type=jnp.float32)) * edge_scale
        message = message.reshape(block_pairs, particles, -1)
        usable = (first_pair + jnp.arange(block_pairs, dtype=jnp.int32))[:, None] < neighbour_count[None, :]
        summed = summed + lax.optimization_barrier(jnp.sum(jnp.where(usable[:, :, None], message, 0.0), axis=0))
    aggregate = summed.astype(jnp.bfloat16)
    node_pre = jnp.dot(latent, node_first[:latent_width], preferred_element_type=jnp.float32) + jnp.dot(aggregate, node_first[latent_width:], preferred_element_type=jnp.float32)
    node_mid = jnp.maximum(node_pre, 0.0).astype(jnp.bfloat16)
    update = layer_norm(jnp.dot(node_mid, node_second, preferred_element_type=jnp.float32)) * node_scale
    return (latent.astype(jnp.float32) + update).astype(jnp.bfloat16)

def direction_table():
    direction = np.arange(27)
    return np.stack([direction // 9 - 1, direction // 3 % 3 - 1, direction % 3 - 1], axis=1)

def neighbour_ids(device):
    shifts = jnp.asarray(direction_table(), dtype=jnp.int32)
    along_first = device // (N_GY * N_GZ) + shifts[:, 0]
    along_second = device // N_GZ % N_GY + shifts[:, 1]
    along_third = device % N_GZ + shifts[:, 2]
    inside = (along_first >= 0) & (along_first < N_GX) & (along_second >= 0) & (along_second < N_GY) & (along_third >= 0) & (along_third < N_GZ)
    other_id = (jnp.clip(along_first, 0, N_GX - 1) * N_GY + jnp.clip(along_second, 0, N_GY - 1)) * N_GZ + jnp.clip(along_third, 0, N_GZ - 1)
    return (other_id.astype(jnp.int32), inside)

def reference(kinematics, pair_offsets, pair_index, neighbour_count, send_rows, migrate_dir, migrate_slot, enc_node_w1, enc_node_w2, enc_edge_w1, enc_edge_w2, edge_w1, edge_w2, node_w1, node_w2, edge_gain, node_gain, dec_w1, dec_w2):
    device_total = N_GX * N_GY * N_GZ
    latent_width = enc_node_w2.shape[1]
    node_hidden = jnp.maximum(jnp.einsum('cn,ch->nh', kinematics[3:], enc_node_w1, precision=lax.Precision.HIGHEST), 0.0).astype(jnp.bfloat16)
    latent = layer_norm(jnp.dot(node_hidden, enc_node_w2, preferred_element_type=jnp.float32)).astype(jnp.bfloat16)
    latent = latent.reshape(device_total, PART_DEV, latent_width)
    offsets_split = pair_offsets.reshape(3, K, device_total, PART_DEV)
    pairs_split = pair_index.reshape(K, device_total, PART_DEV)
    counts_split = neighbour_count.reshape(device_total, PART_DEV)
    sends_split = send_rows.reshape(27, device_total, GHOST)
    backward = (26 - jnp.arange(27, dtype=jnp.int32)).astype(jnp.int32)
    for round_index in range(ROUNDS):

        def advance(device, latent=latent, round_index=round_index):
            other_id, inside = neighbour_ids(device)
            picked = sends_split[backward, other_id]
            ghosts = latent[other_id[:, None], picked]
            ghosts = jnp.where(inside[:, None, None], ghosts, jnp.zeros_like(ghosts))
            extended = jnp.concatenate([latent[device], ghosts.reshape(27 * GHOST, latent_width)], axis=0)
            edge_latent = encode_edges(offsets_split[:, :, device], enc_edge_w1, enc_edge_w2)
            return message_round(latent[device], extended, edge_latent, pairs_split[:, device], counts_split[device], edge_w1[round_index], edge_w2[round_index], node_w1[round_index], node_w2[round_index], edge_gain[round_index], node_gain[round_index], K)
        latent = lax.map(advance, jnp.arange(device_total, dtype=jnp.int32))
    flat_latent = latent.reshape(device_total * PART_DEV, latent_width)
    decode_hidden = jnp.maximum(jnp.dot(flat_latent, dec_w1, preferred_element_type=jnp.float32), 0.0).astype(jnp.bfloat16)
    acceleration = jnp.einsum('ch,nh->cn', dec_w2, decode_hidden.astype(jnp.float32), precision=lax.Precision.HIGHEST)
    velocity = kinematics[STATE - 3:] + acceleration
    new_state = jnp.concatenate([kinematics[:3] + velocity, kinematics[6:], velocity], axis=0)
    staying = migrate_dir == 13
    stayed = jnp.where(staying[None, :], new_state, 0.0)
    owner_device = (jnp.arange(device_total * PART_DEV, dtype=jnp.int32) // PART_DEV).astype(jnp.int32)
    target = jnp.where(staying, 27, migrate_dir).astype(jnp.int32)
    mailbox = jnp.zeros((device_total, 28, MIG, STATE), jnp.float32).at[owner_device, target, migrate_slot.astype(jnp.int32)].set(new_state.T)
    other_all, inside_all = jax.vmap(neighbour_ids)(jnp.arange(device_total, dtype=jnp.int32))
    received = mailbox[other_all, backward[None, :]]
    received = jnp.where(inside_all[:, :, None, None], received, 0.0)
    arrived = received.reshape(device_total * 27 * MIG, STATE).T
    return (stayed, arrived)
```

```python
import functools

import jax
import jax.numpy as jnp
from jax import lax
from jax.experimental import pallas as pl
from jax.experimental.pallas import tpu as pltpu
from jax.sharding import PartitionSpec as P

MIG = 4

norm_eps = 1e-05
F32 = jnp.float32
BF16 = jnp.bfloat16
I32 = jnp.int32
MESH = pl.DeviceIdType.MESH
AXES = ("gx", "gy", "gz")


def dot(a, b):
    return jnp.dot(a, b, preferred_element_type=F32)


def dot_nt(a, b):
    return lax.dot_general(a, b, (((1,), (1,)), ((), ())), preferred_element_type=F32)


def iota(shape, axis):
    return lax.broadcasted_iota(I32, shape, axis)


def head(values):
    return values.astype(BF16).astype(F32)


def inverse_spread(square_sum, width):
    return lax.rsqrt(square_sum * (1.0 / width) + norm_eps)


def fold_rows(values):
    rows, lanes = values.shape
    return jnp.sum(values.reshape(rows // 8, 8, lanes), axis=0)


def normed(center):
    return center * inverse_spread(jnp.sum(center * center, axis=0, keepdims=True), center.shape[0])


class Slots:
    def __init__(self, sizes):
        self.folded = sizes[0] == 2
        steps = [(q // 9 - 1, q // 3 % 3 - 1, q % 3 - 1) for q in range(27) if q != 13]
        if self.folded:
            steps = [s for s in steps if s[0] >= 0]
        first = (1, 0, 0)
        self.steps = [first] + sorted((s for s in steps if s != first), key=lambda s: -sum(map(abs, s)))
        self.number = {s: n for n, s in enumerate(self.steps)}

    def __len__(self):
        return len(self.steps)

    def opposite(self, n):
        x, y, z = self.steps[n]
        return self.number[(x if self.folded else -x, -y, -z)]

    def direction(self, n):
        x, y, z = self.steps[n]
        rest = (y + 1) * 3 + z + 1
        if self.folded and x == 1:
            return rest + 18 - 18 * lax.axis_index("gx")
        return rest + (x + 1) * 9

    def place(self, n):
        x, y, z = self.steps[n]
        return (x if self.folded else x + 1) * 9 + (y + 1) * 3 + z + 1

    def peer(self, n):
        x, y, z = self.steps[n]
        i, j, k = (lax.axis_index(axis) for axis in AXES)
        there = (1 - i if x else i) if self.folded else i + x, j + y, k + z
        tests = []
        for axis, step, position in zip(AXES, self.steps[n], there):
            if step and not (self.folded and axis == "gx"):
                tests.append(jnp.logical_and(position >= 0, position < lax.axis_size(axis)))
        return there, functools.reduce(jnp.logical_and, tests) if tests else None


def guarded(inside, action):
    if inside is None:
        action()
    else:
        pl.when(inside)(action)


def enter(slots):
    barrier = pltpu.get_barrier_semaphore()
    for n in range(len(slots)):
        there, inside = slots.peer(n)
        guarded(inside, lambda: pl.semaphore_signal(barrier, inc=1, device_id=there, device_id_type=MESH))
    peers = 1
    for axis in AXES:
        i, n = lax.axis_index(axis), lax.axis_size(axis)
        peers = peers * (1 + jnp.where(i > 0, 1, 0) + jnp.where(i < n - 1, 1, 0))
    return barrier, peers - 1


def remote(source, target, send_sem, recv_sem, there):
    return pltpu.make_async_remote_copy(
        src_ref=source, dst_ref=target, send_sem=send_sem, recv_sem=recv_sem,
        device_id=there, device_id_type=MESH,
    )


def send(slots, outbox, inbox, send_sems, recv_sems, by_direction=False):
    for n in list(range(1, len(slots))) + [0]:
        there, inside = slots.peer(n)
        far = slots.opposite(n)
        q = slots.direction(n) if by_direction else n
        into = 26 - q if by_direction else far
        copy = remote(outbox.at[q], inbox.at[into], send_sems.at[n], recv_sems.at[far], there)
        guarded(inside, copy.start)


def land(slots, numbers, outbox, inbox, send_sems, recv_sems, by_direction=False):
    for n in numbers:
        there, inside = slots.peer(n)
        q = slots.direction(n) if by_direction else n
        copy = remote(outbox.at[q], inbox.at[q], send_sems.at[n], recv_sems.at[n], there)

        def both():
            copy.wait_recv()
            copy.wait_send()

        guarded(inside, both)


def encode_nodes(kin_ref, node_w1, node_w2, center_of, square, wide):
    features = node_w1.shape[0]
    square[...] = jnp.zeros_like(square)
    wide[...] = jnp.zeros_like(wide)
    first = node_w1[...]
    square[0:features, :] = first
    square[16 : 16 + features, :] = first
    square[32 : 32 + features, :] = first - head(first)
    moves = kin_ref[3:, :]
    wide[0:features, :] = moves
    wide[16 : 16 + features, :] = moves - head(moves)
    wide[32 : 32 + features, :] = moves
    hidden = jnp.maximum(dot(square[...].T.astype(BF16), wide[...].astype(BF16)), 0.0).astype(BF16)
    second = dot_nt(center_of, node_w2[...]).astype(BF16)
    return normed(dot(second, hidden)).astype(BF16)


def fill_send_hot(slots, send_ref, send_hot):
    ghosts = send_ref.shape[0]
    particles = send_hot.shape[1]
    position = iota((ghosts, particles), 1)
    for n in range(len(slots)):
        x, y, z = slots.steps[n]
        q = slots.place(n) + (9 if slots.folded else 0)
        wanted = send_ref[:, q : q + 1]
        if slots.folded and x == 1:
            wanted = jnp.where(lax.axis_index("gx") == 0, wanted, send_ref[:, q - 18 : q - 17])
        send_hot[n * ghosts : (n + 1) * ghosts, :] = jnp.where(position == wanted, 1.0, 0.0).astype(BF16)


def prepare_indices(slots, index_ref, local_code, ghost_code, row_code, ghosts):
    pair_slots, particles = index_ref.shape
    lanes = row_code.shape[1]
    index = index_ref[...]
    ghost = index - particles
    half = 9 * ghosts
    if slots.folded:
        code = jnp.where(ghost < half, ghost + half, ghost - half) - half
    else:
        code = ghost - 3 * half // 2
    local_code[...] = index.astype(F32)
    ghost_code[...] = jnp.where(index < particles, 255, code).astype(F32)
    steps = iota((16, lanes), 0)
    for b in range(particles // 16):
        row_code[16 * b : 16 * (b + 1), :] = (steps + 16 * b).astype(F32).astype(BF16)
    shift = half if slots.folded else 3 * half // 2
    rows = iota((ghosts, lanes), 0)
    for n in range(len(slots)):
        start = particles + n * ghosts
        row_code[start : start + ghosts, :] = (rows + (slots.place(n) * ghosts - shift)).astype(F32).astype(BF16)


def fill_pair_hot(k, local_code, ghost_code, row_code, near, far, width, ghosts):
    particles = near.shape[2]
    one = jnp.ones((16, particles), BF16)
    zero = jnp.zeros((16, particles), BF16)
    local = jnp.broadcast_to(local_code[pl.ds(k, 1), :], (16, particles)).astype(BF16)
    ghost = jnp.broadcast_to(ghost_code[pl.ds(k, 1), :], (16, particles)).astype(BF16)

    def block(row, code):
        return jnp.where(row_code[row : row + 16, :] == code, one, zero)

    for b in range(particles // 16):
        near[k, 16 * b : 16 * (b + 1), :] = block(16 * b, local)
    for b in range(ghosts // 16):
        start = particles + width + 16 * b
        near[k, start : start + 16, :] = block(particles + 16 * b, ghost)
    for b in range(far.shape[1] // 16):
        far[k, 16 * b : 16 * (b + 1), :] = block(particles + ghosts + 16 * b, ghost)


def edge_features(off_ref, edge_w1, square, feature):
    pair_slots = off_ref.shape[1]
    width = edge_w1.shape[1]
    x, y, z = off_ref[0], off_ref[1], off_ref[2]
    terms = (x, y, z, x * x + y * y + z * z)
    rows = 4 * pair_slots
    for c, term in enumerate(terms):
        high = term.astype(BF16)
        low = (term - high.astype(F32)).astype(BF16)
        feature[c * pair_slots : (c + 1) * pair_slots, :] = high
        feature[rows + c * pair_slots : rows + (c + 1) * pair_slots, :] = low
        feature[2 * rows + c * pair_slots : 2 * rows + (c + 1) * pair_slots, :] = high
    first = edge_w1[...]
    square[0:4, :] = first
    square[4:8, :] = first
    square[8:12, :] = first - head(first)
    spread_row = iota((width, 3 * rows), 0)
    spread_lane = iota((width, 3 * rows), 1)
    spread = jnp.where(spread_lane // pair_slots == spread_row, 1.0, 0.0).astype(BF16)
    return dot(square[...].T.astype(BF16), spread)


def step_kernel(
    kin_ref, off_ref, index_ref, count_ref, send_ref, dir_ref, slot_ref, enc_node_w1, enc_node_w2,
    enc_edge_w1, enc_edge_w2, edge_w1, edge_w2, node_w1, node_w2, edge_gain, node_gain, dec_w1,
    dec_w2, stayed_ref, arrived_ref, outbox, inbox, leaving, landed, send_sems, recv_sems,
    square, wide, feature, base, local_code, ghost_code, row_code, send_hot, near, far,
    hidden, partial, squares, near_left, far_left, received, first_t, second_c, node_t, node_c,
    gains, both, state, rows,
):
    sizes = [lax.axis_size(axis) for axis in AXES]
    slots = Slots(sizes)
    width = enc_node_w2.shape[1]
    state_rows, particles = kin_ref.shape
    pair_slots = index_ref.shape[0]
    ghosts = send_ref.shape[0]
    rounds = edge_w1.shape[0]

    for r in range(rounds):
        inbox[r] = jnp.zeros(inbox.shape[1:], inbox.dtype)
    landed[...] = jnp.zeros_like(landed)
    barrier, peers = enter(slots)

    diagonal = iota((width, width), 0) == iota((width, width), 1)
    unit = jnp.where(diagonal, 1.0, 0.0).astype(BF16)
    center_of = jnp.where(diagonal, 1.0 - 1.0 / width, -1.0 / width).astype(BF16)

    fill_send_hot(slots, send_ref, send_hot)
    latent = encode_nodes(kin_ref, enc_node_w1, enc_node_w2, center_of, square, wide)
    both[0:width, :] = latent
    outbox[0] = dot_nt(send_hot[...], latent).astype(BF16).reshape(outbox.shape[1:])
    pl.semaphore_wait(barrier, peers)

    def path(r):
        return outbox.at[r], inbox.at[r], send_sems.at[r], recv_sems.at[r]

    def turn_weights(r):
        first_t[r] = dot_nt(unit, edge_w1[r]).astype(BF16)
        second_c[r] = dot_nt(center_of, edge_w2[r]).astype(BF16)
        node_t[r] = dot_nt(unit, node_w1[r]).astype(BF16)
        node_c[r] = dot_nt(center_of, node_w2[r]).astype(BF16)

    def local_part(r):
        weights = first_t.at[r]
        now = both[0:width, :]
        received[...] = dot(weights[:, width : 2 * width], now)
        near_left[:, 0:particles] = dot(weights[:, 2 * width :], now).astype(BF16)
        near_left[:, particles : particles + width] = weights[:, 0:width]

    for r in range(rounds):
        send(slots, *path(r))
        if r == 0:
            base[...] = edge_features(off_ref, enc_edge_w1, square, feature).astype(BF16)
            enc_second = dot_nt(center_of, enc_edge_w2[...]).astype(BF16)
            prepare_indices(slots, index_ref, local_code, ghost_code, row_code, ghosts)
            slot_of = iota(base.shape, 1) % pair_slots

            def first_edge(k, carry):
                left = jnp.where(slot_of == k, base[...].astype(F32), 0.0).astype(BF16)
                hidden[k] = jnp.maximum(dot(left, feature[...]), 0.0).astype(BF16)
                return carry

            lax.fori_loop(0, pair_slots, first_edge, 0, unroll=4)

            def second_edge(k, carry):
                fresh = normed(dot(enc_second, hidden[k])).astype(BF16)
                near[k, particles : particles + width, :] = fresh
                fill_pair_hot(k, local_code, ghost_code, row_code, near, far, width, ghosts)
                return carry

            lax.fori_loop(0, pair_slots, second_edge, 0, unroll=4)
            turn_weights(0)
            square[0:rounds, :] = edge_gain[...]
            square[rounds : 2 * rounds, :] = node_gain[...]
            columns = square[...].T
            for g in range(2 * rounds):
                gains[g] = jnp.broadcast_to(columns[:, g : g + 1], (width, width))
        local_part(r)
        land(slots, [0], *path(r))
        first_ghosts = inbox[r, 0]
        near_left[:, particles + width :] = dot_nt(first_t[r, :, 2 * width :], first_ghosts).astype(BF16)

        def early(k, carry):
            partial[k] = dot(near_left[...], near[k]) + received[...]
            return carry

        lax.fori_loop(0, pair_slots, early, 0, unroll=4)
        if r + 1 < rounds:
            turn_weights(r + 1)
        land(slots, range(1, len(slots)), *path(r))
        late_ghosts = inbox[r, 1:].reshape(-1, width)
        far_left[...] = dot_nt(first_t[r, :, 2 * width :], late_ghosts).astype(BF16)

        def late(k, carry):
            hidden[k] = jnp.maximum(partial[k] + dot(far_left[...], far[k]), 0.0).astype(BF16)
            return carry

        lax.fori_loop(0, pair_slots, late, 0, unroll=4)

        def second(k, carry):
            center = dot(second_c[r], hidden[k])
            partial[k] = center
            scale = inverse_spread(jnp.sum(center * center, axis=0, keepdims=True), width)
            squares[k] = jnp.broadcast_to(jnp.where(k < count_ref[...], scale, 0.0), squares.shape[1:])
            return carry

        lax.fori_loop(0, pair_slots, second, 0, unroll=4)

        edge_column = jnp.concatenate([gains[r]] * (particles // width), axis=1)
        node_column = jnp.concatenate([gains[rounds + r]] * (particles // width), axis=1)
        for f in range(0, width, 8):
            total = partial[0, f : f + 8, :] * squares[0]
            for k in range(1, pair_slots):
                total = total + partial[k, f : f + 8, :] * squares[k]
            received[f : f + 8, :] = total
        both[width : 2 * width, :] = (received[...] * edge_column).astype(BF16)
        middle = jnp.maximum(dot(node_t[r], both[...]), 0.0).astype(BF16)
        update = normed(dot(node_c[r], middle)) * node_column
        latent = (both[0:width, :].astype(F32) + update).astype(BF16)
        both[0:width, :] = latent
        if r + 1 < rounds:
            outbox[r + 1] = dot_nt(send_hot[...], latent).astype(BF16).reshape(outbox.shape[1:])

    reading = dec_w2[...]
    wide[...] = jnp.zeros_like(wide)
    wide[0:3, 0:width] = reading
    wide[8:11, 0:width] = reading - head(reading)
    wide[16:19, 0:width] = reading - head(reading) - head(reading - head(reading))
    readout = wide[0:32, 0:width].astype(BF16)
    decoded = jnp.maximum(dot(dot_nt(unit, dec_w1[...]).astype(BF16), latent), 0.0).astype(BF16)
    parts = dot(readout, decoded)
    velocity = kin_ref[state_rows - 3 :, :] + (parts[0:3, :] + (parts[8:11, :] + parts[16:19, :]))
    state[...] = jnp.zeros_like(state)
    state[0:3, :] = kin_ref[0:3, :] + velocity
    state[3 : state_rows - 3, :] = kin_ref[6:, :]
    state[state_rows - 3 : state_rows, :] = velocity
    staying = dir_ref[...] == 13
    target = jnp.where(staying, -1, dir_ref[...] * MIG + slot_ref[...])
    picker = jnp.where(iota((rows.shape[0], particles), 0) == target, 1.0, 0.0).astype(BF16)
    whole = state[...]
    high = whole.astype(BF16)
    rest = whole - high.astype(F32)
    middle = rest.astype(BF16)
    low = (rest - middle.astype(F32)).astype(BF16)
    rows[:, 0 : state.shape[0]] = dot_nt(picker, high) + dot_nt(picker, middle) + dot_nt(picker, low)
    for q in range(27):
        leaving[q] = rows[MIG * q : MIG * (q + 1), :]
    migration = (leaving, landed, send_sems.at[rounds], recv_sems.at[rounds])
    send(slots, *migration, by_direction=True)
    stayed_ref[...] = jnp.where(staying, state[0:state_rows, :], 0.0)
    land(slots, range(len(slots)), *migration, by_direction=True)
    for q in range(27):
        rows[MIG * q : MIG * (q + 1), :] = landed[q]
    arrived_ref[...] = rows[...].T[0:state_rows, 0 : 27 * MIG]


def on_device(
    kinematics, pair_offsets, pair_index, neighbour_count, send_rows, migrate_dir, migrate_slot,
    enc_node_w1, enc_node_w2, enc_edge_w1, enc_edge_w2, edge_w1, edge_w2, node_w1, node_w2,
    edge_gain, node_gain, dec_w1, dec_w2,
):
    width = enc_node_w2.shape[1]
    pair_slots, particles = pair_index.shape
    ghosts = send_rows.shape[1]
    state_rows = kinematics.shape[0]
    rounds = edge_w1.shape[0]
    slot_count = len(Slots([lax.axis_size(axis) for axis in AXES]))
    near_rows = particles + width + ghosts
    far_rows = (slot_count - 1) * ghosts
    operands = (
        kinematics, pair_offsets, pair_index, neighbour_count.reshape(1, particles), send_rows.T,
        migrate_dir.reshape(1, particles), migrate_slot.reshape(1, particles), enc_node_w1,
        enc_node_w2, enc_edge_w1, enc_edge_w2, edge_w1, edge_w2, node_w1, node_w2, edge_gain,
        node_gain, dec_w1, dec_w2,
    )
    vmem = pl.BlockSpec(memory_space=pltpu.VMEM)
    return tuple(
        pl.pallas_call(
            step_kernel,
            name="step",
            in_specs=[vmem] * len(operands),
            out_specs=[vmem, vmem],
            out_shape=[
                jax.ShapeDtypeStruct((state_rows, particles), F32),
                jax.ShapeDtypeStruct((state_rows, 27 * MIG), F32),
            ],
            scratch_shapes=[
                pltpu.VMEM((rounds, slot_count, ghosts, width), BF16),
                pltpu.VMEM((rounds, slot_count, ghosts, width), BF16),
                pltpu.VMEM((27, MIG, width), F32),
                pltpu.VMEM((27, MIG, width), F32),
                pltpu.SemaphoreType.DMA((rounds + 1, slot_count)),
                pltpu.SemaphoreType.DMA((rounds + 1, slot_count)),
                pltpu.VMEM((width, width), F32),
                pltpu.VMEM((width, particles), F32),
                pltpu.VMEM((12 * pair_slots, particles), BF16),
                pltpu.VMEM((width, 12 * pair_slots), BF16),
                pltpu.VMEM((pair_slots, particles), F32),
                pltpu.VMEM((pair_slots, particles), F32),
                pltpu.VMEM((particles + slot_count * ghosts, particles), BF16),
                pltpu.VMEM((slot_count * ghosts, particles), BF16),
                pltpu.VMEM((pair_slots, near_rows, particles), BF16),
                pltpu.VMEM((pair_slots, far_rows, particles), BF16),
                pltpu.VMEM((pair_slots, width, particles), BF16),
                pltpu.VMEM((pair_slots, width, particles), F32),
                pltpu.VMEM((pair_slots, 8, particles), F32),
                pltpu.VMEM((width, near_rows), BF16),
                pltpu.VMEM((width, far_rows), BF16),
                pltpu.VMEM((width, particles), F32),
                pltpu.VMEM((rounds, width, 3 * width), BF16),
                pltpu.VMEM((rounds, width, width), BF16),
                pltpu.VMEM((rounds, width, 2 * width), BF16),
                pltpu.VMEM((rounds, width, width), BF16),
                pltpu.VMEM((2 * rounds, width, width), F32),
                pltpu.VMEM((2 * width, particles), BF16),
                pltpu.VMEM((32, particles), F32),
                pltpu.VMEM((width, width), F32),
            ],
            compiler_params=pltpu.CompilerParams(collective_id=0, has_side_effects=True),
        )(*operands)
    )


def solution(mesh):
    split = ("gx", "gy", "gz")
    return jax.shard_map(
        on_device,
        mesh=mesh,
        in_specs=(
            P(None, split),
            P(None, None, split),
            P(None, split),
            P(split),
            P(None, split),
            P(split),
            P(split),
        )
        + (P(),) * 12,
        out_specs=(P(None, split), P(None, split)),
        check_vma=False,
    )
```

```python
import functools

import jax
import jax.numpy as jnp
from jax import lax
from jax.experimental import pallas as pl
from jax.experimental.pallas import tpu as pltpu
from jax.sharding import PartitionSpec as P

MIG = 4

norm_eps = 1e-05
F32 = jnp.float32
BF16 = jnp.bfloat16
I32 = jnp.int32
MESH = pl.DeviceIdType.MESH
AXES = ("gx", "gy", "gz")


def dot(a, b):
    return jnp.dot(a, b, preferred_element_type=F32)


def dot_nt(a, b):
    return lax.dot_general(a, b, (((1,), (1,)), ((), ())), preferred_element_type=F32)


def iota(shape, axis):
    return lax.broadcasted_iota(I32, shape, axis)


def head(values):
    return values.astype(BF16).astype(F32)


def inverse_spread(square_sum, width):
    return lax.rsqrt(square_sum * (1.0 / width) + norm_eps)


def fold_rows(values):
    rows, lanes = values.shape
    return jnp.sum(values.reshape(rows // 8, 8, lanes), axis=0)


def normed(center):
    return center * inverse_spread(jnp.sum(center * center, axis=0, keepdims=True), center.shape[0])


class Slots:
    def __init__(self, sizes):
        self.folded = sizes[0] == 2
        steps = [(q // 9 - 1, q // 3 % 3 - 1, q % 3 - 1) for q in range(27) if q != 13]
        if self.folded:
            steps = [s for s in steps if s[0] >= 0]
        hops = lambda step: sum(map(abs, step))
        self.steps = sorted(steps, key=hops)
        self.faces = sum(hops(step) == 1 for step in steps)
        self.number = {s: n for n, s in enumerate(self.steps)}

    def __len__(self):
        return len(self.steps)

    def opposite(self, n):
        x, y, z = self.steps[n]
        return self.number[(x if self.folded else -x, -y, -z)]

    def direction(self, n):
        x, y, z = self.steps[n]
        rest = (y + 1) * 3 + z + 1
        if self.folded and x == 1:
            return rest + 18 - 18 * lax.axis_index("gx")
        return rest + (x + 1) * 9

    def place(self, n):
        x, y, z = self.steps[n]
        return (x if self.folded else x + 1) * 9 + (y + 1) * 3 + z + 1

    def peer(self, n):
        x, y, z = self.steps[n]
        i, j, k = (lax.axis_index(axis) for axis in AXES)
        there = (1 - i if x else i) if self.folded else i + x, j + y, k + z
        tests = []
        for axis, step, position in zip(AXES, self.steps[n], there):
            if step and not (self.folded and axis == "gx"):
                tests.append(jnp.logical_and(position >= 0, position < lax.axis_size(axis)))
        return there, functools.reduce(jnp.logical_and, tests) if tests else None


def guarded(inside, action):
    if inside is None:
        action()
    else:
        pl.when(inside)(action)


def clear(slots, inbox, landed):
    for n in range(len(slots)):
        inside = slots.peer(n)[1]
        if inside is not None:

            @pl.when(jnp.logical_not(inside))
            def _():
                for r in range(inbox.shape[0]):
                    inbox[r, n] = jnp.zeros(inbox.shape[2:], inbox.dtype)

    position = [lax.axis_index(axis) for axis in AXES]
    for q in range(27):
        tests = [jnp.full((), q == 13)]
        for i, axis, step in zip(position, AXES, (q // 9 - 1, q // 3 % 3 - 1, q % 3 - 1)):
            if step:
                tests.append(i == (0 if step < 0 else lax.axis_size(axis) - 1))

        @pl.when(functools.reduce(jnp.logical_or, tests))
        def _():
            landed[q] = jnp.zeros(landed.shape[1:], landed.dtype)


def enter(slots):
    barrier = pltpu.get_barrier_semaphore()
    for n in range(len(slots)):
        there, inside = slots.peer(n)
        guarded(inside, lambda: pl.semaphore_signal(barrier, inc=1, device_id=there, device_id_type=MESH))
    peers = 1
    for axis in AXES:
        i, n = lax.axis_index(axis), lax.axis_size(axis)
        peers = peers * (1 + jnp.where(i > 0, 1, 0) + jnp.where(i < n - 1, 1, 0))
    return barrier, peers - 1


def remote(source, target, send_sem, recv_sem, there):
    return pltpu.make_async_remote_copy(
        src_ref=source, dst_ref=target, send_sem=send_sem, recv_sem=recv_sem,
        device_id=there, device_id_type=MESH,
    )


def send(slots, outbox, inbox, send_sems, recv_sems, by_direction=False):
    for n in reversed(range(len(slots))):
        there, inside = slots.peer(n)
        far = slots.opposite(n)
        q = slots.direction(n) if by_direction else n
        into = 26 - q if by_direction else far
        copy = remote(outbox.at[q], inbox.at[into], send_sems.at[n], recv_sems.at[far], there)
        guarded(inside, copy.start)


def land(slots, numbers, outbox, inbox, send_sems, recv_sems, by_direction=False):
    for n in numbers:
        there, inside = slots.peer(n)
        q = slots.direction(n) if by_direction else n
        copy = remote(outbox.at[q], inbox.at[q], send_sems.at[n], recv_sems.at[n], there)

        def both():
            copy.wait_recv()
            copy.wait_send()

        guarded(inside, both)


def encode_nodes(kin_ref, node_w1, node_w2, center_of, square, wide):
    features = node_w1.shape[0]
    square[...] = jnp.zeros_like(square)
    wide[...] = jnp.zeros_like(wide)
    first = node_w1[...]
    square[0:features, :] = first
    square[16 : 16 + features, :] = first
    square[32 : 32 + features, :] = first - head(first)
    moves = kin_ref[3:, :]
    wide[0:features, :] = moves
    wide[16 : 16 + features, :] = moves - head(moves)
    wide[32 : 32 + features, :] = moves
    hidden = jnp.maximum(dot(square[...].T.astype(BF16), wide[...].astype(BF16)), 0.0).astype(BF16)
    second = dot_nt(center_of, node_w2[...]).astype(BF16)
    return normed(dot(second, hidden)).astype(BF16)


def fill_send_hot(slots, send_ref, send_hot):
    ghosts = send_ref.shape[0]
    particles = send_hot.shape[1]
    position = iota((ghosts, particles), 1)
    for n in range(len(slots)):
        x, y, z = slots.steps[n]
        q = slots.place(n) + (9 if slots.folded else 0)
        wanted = send_ref[:, q : q + 1]
        if slots.folded and x == 1:
            wanted = jnp.where(lax.axis_index("gx") == 0, wanted, send_ref[:, q - 18 : q - 17])
        send_hot[n * ghosts : (n + 1) * ghosts, :] = jnp.where(position == wanted, 1.0, 0.0).astype(BF16)


def prepare_indices(slots, index_ref, local_code, ghost_code, row_code, ghosts):
    pair_slots, particles = index_ref.shape
    lanes = row_code.shape[1]
    index = index_ref[...]
    ghost = index - particles
    half = 9 * ghosts
    if slots.folded:
        code = jnp.where(ghost < half, ghost + half, ghost - half) - half
    else:
        code = ghost - 3 * half // 2
    local_code[...] = index.astype(F32)
    ghost_code[...] = jnp.where(index < particles, 255, code).astype(F32)
    steps = iota((16, lanes), 0)
    for b in range(particles // 16):
        row_code[16 * b : 16 * (b + 1), :] = (steps + 16 * b).astype(F32).astype(BF16)
    shift = half if slots.folded else 3 * half // 2
    rows = iota((ghosts, lanes), 0)
    for n in range(len(slots)):
        start = particles + n * ghosts
        row_code[start : start + ghosts, :] = (rows + (slots.place(n) * ghosts - shift)).astype(F32).astype(BF16)


def fill_pair_hot(k, local_code, ghost_code, row_code, own, near, far, width):
    particles = near.shape[2]
    near_ghosts = near.shape[1] - width
    one = jnp.ones((16, particles), BF16)
    zero = jnp.zeros((16, particles), BF16)
    local = jnp.broadcast_to(local_code[pl.ds(k, 1), :], (16, particles)).astype(BF16)
    ghost = jnp.broadcast_to(ghost_code[pl.ds(k, 1), :], (16, particles)).astype(BF16)

    def block(row, code):
        return jnp.where(row_code[row : row + 16, :] == code, one, zero)

    for b in range(particles // 16):
        own[k, 16 * b : 16 * (b + 1), :] = block(16 * b, local)
    for b in range(near_ghosts // 16):
        start = width + 16 * b
        near[k, start : start + 16, :] = block(particles + 16 * b, ghost)
    for b in range(far.shape[1] // 16):
        far[k, 16 * b : 16 * (b + 1), :] = block(particles + near_ghosts + 16 * b, ghost)


def edge_features(off_ref, edge_w1, square, feature):
    pair_slots = off_ref.shape[1]
    width = edge_w1.shape[1]
    x, y, z = off_ref[0], off_ref[1], off_ref[2]
    terms = (x, y, z, x * x + y * y + z * z)
    rows = 4 * pair_slots
    for c, term in enumerate(terms):
        high = term.astype(BF16)
        low = (term - high.astype(F32)).astype(BF16)
        feature[c * pair_slots : (c + 1) * pair_slots, :] = high
        feature[rows + c * pair_slots : rows + (c + 1) * pair_slots, :] = low
        feature[2 * rows + c * pair_slots : 2 * rows + (c + 1) * pair_slots, :] = high
    first = edge_w1[...]
    square[0:4, :] = first
    square[4:8, :] = first
    square[8:12, :] = first - head(first)
    spread_row = iota((width, 3 * rows), 0)
    spread_lane = iota((width, 3 * rows), 1)
    spread = jnp.where(spread_lane // pair_slots == spread_row, 1.0, 0.0).astype(BF16)
    return dot(square[...].T.astype(BF16), spread)


def step_kernel(slots, *refs):
    operands, results, scratch = refs[:19], refs[19:21], refs[21:]
    (
        kin_ref, off_ref, index_ref, count_ref, send_ref, dir_ref, slot_ref, enc_node_w1, enc_node_w2,
        enc_edge_w1, enc_edge_w2, edge_w1, edge_w2, node_w1, node_w2, edge_gain, node_gain, dec_w1,
        dec_w2,
    ) = copies = scratch[:19]
    stayed_ref, arrived_ref = results
    (
        copy_sems, outbox, inbox, leaving, landed, send_sems, recv_sems, square, wide, feature, base,
        local_code, ghost_code, row_code, send_hot, own, near, far, hidden, partial, squares, own_left,
        near_left, far_left, received, first_t, second_c, node_t, node_c, gains, both, state, rows,
    ) = scratch[19:]
    width = enc_node_w2.shape[1]
    state_rows, particles = kin_ref.shape
    pair_slots = index_ref.shape[0]
    ghosts = send_ref.shape[0]
    rounds = edge_w1.shape[0]
    faces = slots.faces

    barrier, peers = enter(slots)
    fetches = [
        pltpu.make_async_copy(source, target, copy_sems.at[n])
        for n, (source, target) in enumerate(zip(operands, copies))
    ]
    urgent = [4, 0, 7, 8]
    for n in urgent + [n for n in range(19) if n not in urgent]:
        fetches[n].start()
    clear(slots, inbox, landed)

    diagonal = iota((width, width), 0) == iota((width, width), 1)
    unit = jnp.where(diagonal, 1.0, 0.0).astype(BF16)
    center_of = jnp.where(diagonal, 1.0 - 1.0 / width, -1.0 / width).astype(BF16)

    for n in urgent:
        fetches[n].wait()
    fill_send_hot(slots, send_ref, send_hot)
    latent = encode_nodes(kin_ref, enc_node_w1, enc_node_w2, center_of, square, wide)
    both[0:width, :] = latent
    outbox[0] = dot_nt(send_hot[...], latent).astype(BF16).reshape(outbox.shape[1:])
    pl.semaphore_wait(barrier, peers)

    def path(r):
        return outbox.at[r], inbox.at[r], send_sems.at[r], recv_sems.at[r]

    def turn_weights(r):
        first_t[r] = dot_nt(unit, edge_w1[r]).astype(BF16)
        second_c[r] = dot_nt(center_of, edge_w2[r]).astype(BF16)
        node_t[r] = dot_nt(unit, node_w1[r]).astype(BF16)
        node_c[r] = dot_nt(center_of, node_w2[r]).astype(BF16)

    def local_part(r):
        weights = first_t.at[r]
        now = both[0:width, :]
        received[...] = dot(weights[:, width : 2 * width], now)
        own_left[...] = dot(weights[:, 2 * width :], now).astype(BF16)
        near_left[:, 0:width] = weights[:, 0:width]

    for r in range(rounds):
        send(slots, *path(r))
        if r == 0:
            for n in range(19):
                if n not in urgent:
                    fetches[n].wait()
            base[...] = edge_features(off_ref, enc_edge_w1, square, feature).astype(BF16)
            enc_second = dot_nt(center_of, enc_edge_w2[...]).astype(BF16)
            prepare_indices(slots, index_ref, local_code, ghost_code, row_code, ghosts)
            slot_of = iota(base.shape, 1) % pair_slots

            def first_edge(k, carry):
                left = jnp.where(slot_of == k, base[...].astype(F32), 0.0).astype(BF16)
                hidden[k] = jnp.maximum(dot(left, feature[...]), 0.0).astype(BF16)
                return carry

            lax.fori_loop(0, pair_slots, first_edge, 0, unroll=pair_slots)

            def second_edge(k, carry):
                fresh = normed(dot(enc_second, hidden[k])).astype(BF16)
                near[k, 0:width, :] = fresh
                fill_pair_hot(k, local_code, ghost_code, row_code, own, near, far, width)
                return carry

            lax.fori_loop(0, pair_slots, second_edge, 0, unroll=pair_slots)
            turn_weights(0)
            square[0:rounds, :] = edge_gain[...]
            square[rounds : 2 * rounds, :] = node_gain[...]
            columns = square[...].T
            for g in range(2 * rounds):
                gains[g] = jnp.broadcast_to(columns[:, g : g + 1], (width, width))
        local_part(r)

        def local(k, carry):
            partial[k] = dot(own_left[...], own[k]) + received[...]
            return carry

        lax.fori_loop(0, pair_slots, local, 0, unroll=pair_slots)
        if r + 1 < rounds:
            turn_weights(r + 1)
        land(slots, range(faces), *path(r))
        near_left[:, width:] = dot_nt(
            first_t[r, :, 2 * width :], inbox[r, 0:faces].reshape(-1, width)
        ).astype(BF16)

        def early(k, carry):
            partial[k] = partial[k] + dot(near_left[...], near[k])
            return carry

        lax.fori_loop(0, pair_slots, early, 0, unroll=pair_slots)
        land(slots, range(faces, len(slots)), *path(r))
        far_left[...] = dot_nt(
            first_t[r, :, 2 * width :], inbox[r, faces:].reshape(-1, width)
        ).astype(BF16)
        edge_column = jnp.concatenate([gains[r]] * (particles // width), axis=1)
        node_column = jnp.concatenate([gains[rounds + r]] * (particles // width), axis=1)
        group = 4
        for start in range(0, pair_slots, group):
            members = range(start, start + group)
            for k in members:
                hidden[k] = jnp.maximum(partial[k] + dot(far_left[...], far[k]), 0.0).astype(BF16)
            for k in members:
                center = dot(second_c[r], hidden[k])
                partial[k] = center
                scale = inverse_spread(jnp.sum(center * center, axis=0, keepdims=True), width)
                scale = jnp.where(k < count_ref[...], scale, 0.0)
                squares[k] = jnp.broadcast_to(scale, squares.shape[1:])
            for f in range(0, width, 8):
                total = functools.reduce(
                    jnp.add, [partial[k, f : f + 8, :] * squares[k] for k in members]
                )
                received[f : f + 8, :] = total + received[f : f + 8, :] if start else total

        both[width : 2 * width, :] = (received[...] * edge_column).astype(BF16)
        middle = jnp.maximum(dot(node_t[r], both[...]), 0.0).astype(BF16)
        update = normed(dot(node_c[r], middle)) * node_column
        latent = (both[0:width, :].astype(F32) + update).astype(BF16)
        both[0:width, :] = latent
        if r + 1 < rounds:
            outbox[r + 1] = dot_nt(send_hot[...], latent).astype(BF16).reshape(outbox.shape[1:])

    reading = dec_w2[...]
    wide[...] = jnp.zeros_like(wide)
    wide[0:3, 0:width] = reading
    wide[8:11, 0:width] = reading - head(reading)
    wide[16:19, 0:width] = reading - head(reading) - head(reading - head(reading))
    readout = wide[0:32, 0:width].astype(BF16)
    decoded = jnp.maximum(dot(dot_nt(unit, dec_w1[...]).astype(BF16), latent), 0.0).astype(BF16)
    parts = dot(readout, decoded)
    velocity = kin_ref[state_rows - 3 :, :] + (parts[0:3, :] + (parts[8:11, :] + parts[16:19, :]))
    state[...] = jnp.zeros_like(state)
    state[0:3, :] = kin_ref[0:3, :] + velocity
    state[3 : state_rows - 3, :] = kin_ref[6:, :]
    state[state_rows - 3 : state_rows, :] = velocity
    staying = dir_ref[...] == 13
    target = jnp.where(staying, -1, dir_ref[...] * MIG + slot_ref[...])
    picker = jnp.where(iota((rows.shape[0], particles), 0) == target, 1.0, 0.0).astype(BF16)
    whole = state[...]
    high = whole.astype(BF16)
    rest = whole - high.astype(F32)
    middle = rest.astype(BF16)
    low = (rest - middle.astype(F32)).astype(BF16)
    rows[:, 0 : state.shape[0]] = dot_nt(picker, high) + dot_nt(picker, middle) + dot_nt(picker, low)
    for q in range(27):
        leaving[q] = rows[MIG * q : MIG * (q + 1), :]
    migration = (leaving, landed, send_sems.at[rounds], recv_sems.at[rounds])
    send(slots, *migration, by_direction=True)
    stayed_ref[...] = jnp.where(staying, state[0:state_rows, :], 0.0)
    land(slots, range(len(slots)), *migration, by_direction=True)
    for q in range(27):
        rows[MIG * q : MIG * (q + 1), :] = landed[q]
    arrived_ref[...] = rows[...].T[0:state_rows, 0 : 27 * MIG]


def on_device(
    kinematics, pair_offsets, pair_index, neighbour_count, send_rows, migrate_dir, migrate_slot,
    enc_node_w1, enc_node_w2, enc_edge_w1, enc_edge_w2, edge_w1, edge_w2, node_w1, node_w2,
    edge_gain, node_gain, dec_w1, dec_w2,
):
    width = enc_node_w2.shape[1]
    pair_slots, particles = pair_index.shape
    ghosts = send_rows.shape[1]
    state_rows = kinematics.shape[0]
    rounds = edge_w1.shape[0]
    slots = Slots([lax.axis_size(axis) for axis in AXES])
    count = len(slots)
    near_rows = width + slots.faces * ghosts
    far_rows = (count - slots.faces) * ghosts
    operands = (
        kinematics, pair_offsets, pair_index, neighbour_count.reshape(1, particles), send_rows.T,
        migrate_dir.reshape(1, particles), migrate_slot.reshape(1, particles), enc_node_w1,
        enc_node_w2, enc_edge_w1, enc_edge_w2, edge_w1, edge_w2, node_w1, node_w2, edge_gain,
        node_gain, dec_w1, dec_w2,
    )
    vmem = pl.BlockSpec(memory_space=pltpu.VMEM)
    anywhere = pl.BlockSpec(memory_space=pl.ANY)
    shapes = [(state_rows, particles), (state_rows, 27 * MIG)]
    found = pl.pallas_call(
        functools.partial(step_kernel, slots),
        name="step",
        in_specs=[anywhere] * len(operands),
        out_specs=[vmem, vmem],
        out_shape=[pltpu.VMEM(shape, F32) for shape in shapes],
        scratch_shapes=[pltpu.VMEM(operand.shape, operand.dtype) for operand in operands]
        + [
            pltpu.SemaphoreType.DMA((len(operands),)),
            pltpu.VMEM((rounds, count, ghosts, width), BF16),
            pltpu.VMEM((rounds, count, ghosts, width), BF16),
            pltpu.VMEM((27, MIG, width), F32),
            pltpu.VMEM((27, MIG, width), F32),
            pltpu.SemaphoreType.DMA((rounds + 1, count)),
            pltpu.SemaphoreType.DMA((rounds + 1, count)),
            pltpu.VMEM((width, width), F32),
            pltpu.VMEM((width, particles), F32),
            pltpu.VMEM((12 * pair_slots, particles), BF16),
            pltpu.VMEM((width, 12 * pair_slots), BF16),
            pltpu.VMEM((pair_slots, particles), F32),
            pltpu.VMEM((pair_slots, particles), F32),
            pltpu.VMEM((particles + count * ghosts, particles), BF16),
            pltpu.VMEM((count * ghosts, particles), BF16),
            pltpu.VMEM((pair_slots, particles, particles), BF16),
            pltpu.VMEM((pair_slots, near_rows, particles), BF16),
            pltpu.VMEM((pair_slots, far_rows, particles), BF16),
            pltpu.VMEM((pair_slots, width, particles), BF16),
            pltpu.VMEM((pair_slots, width, particles), F32),
            pltpu.VMEM((pair_slots, 8, particles), F32),
            pltpu.VMEM((width, particles), BF16),
            pltpu.VMEM((width, near_rows), BF16),
            pltpu.VMEM((width, far_rows), BF16),
            pltpu.VMEM((width, particles), F32),
            pltpu.VMEM((rounds, width, 3 * width), BF16),
            pltpu.VMEM((rounds, width, width), BF16),
            pltpu.VMEM((rounds, width, 2 * width), BF16),
            pltpu.VMEM((rounds, width, width), BF16),
            pltpu.VMEM((2 * rounds, width, width), F32),
            pltpu.VMEM((2 * width, particles), BF16),
            pltpu.VMEM((32, particles), F32),
            pltpu.VMEM((width, width), F32),
        ],
        compiler_params=pltpu.CompilerParams(collective_id=0, has_side_effects=True),
    )(*operands)
    return tuple(found)


def solution(mesh):
    split = ("gx", "gy", "gz")
    return jax.shard_map(
        on_device,
        mesh=mesh,
        in_specs=(
            P(None, split),
            P(None, None, split),
            P(None, split),
            P(split),
            P(None, split),
            P(split),
            P(split),
        )
        + (P(),) * 12,
        out_specs=(P(None, split), P(None, split)),
        check_vma=False,
    )
```

```python
import functools

import jax
import jax.numpy as jnp
from jax import lax
from jax.experimental import pallas as pl
from jax.experimental.pallas import tpu as pltpu
from jax.sharding import PartitionSpec as P

MIG = 4

norm_eps = 1e-05
F32 = jnp.float32
BF16 = jnp.bfloat16
I32 = jnp.int32
MESH = pl.DeviceIdType.MESH
AXES = ("gx", "gy", "gz")


def dot(a, b):
    return jnp.dot(a, b, preferred_element_type=F32)


def dot_nt(a, b):
    return lax.dot_general(a, b, (((1,), (1,)), ((), ())), preferred_element_type=F32)


def iota(shape, axis):
    return lax.broadcasted_iota(I32, shape, axis)


def head(values):
    return values.astype(BF16).astype(F32)


def inverse_spread(square_sum, width):
    return lax.rsqrt(square_sum * (1.0 / width) + norm_eps)


def fold_rows(values):
    rows, lanes = values.shape
    return jnp.sum(values.reshape(rows // 8, 8, lanes), axis=0)


def normed(center):
    return center * inverse_spread(jnp.sum(center * center, axis=0, keepdims=True), center.shape[0])


class Slots:
    def __init__(self, sizes):
        self.folded = sizes[0] == 2
        steps = [(q // 9 - 1, q // 3 % 3 - 1, q % 3 - 1) for q in range(27) if q != 13]
        if self.folded:
            steps = [s for s in steps if s[0] >= 0]
        hops = lambda step: sum(map(abs, step))
        self.steps = sorted(steps, key=hops)
        self.faces = sum(hops(step) == 1 for step in steps)
        self.number = {s: n for n, s in enumerate(self.steps)}

    def __len__(self):
        return len(self.steps)

    def opposite(self, n):
        x, y, z = self.steps[n]
        return self.number[(x if self.folded else -x, -y, -z)]

    def direction(self, n):
        x, y, z = self.steps[n]
        rest = (y + 1) * 3 + z + 1
        if self.folded and x == 1:
            return rest + 18 - 18 * lax.axis_index("gx")
        return rest + (x + 1) * 9

    def place(self, n):
        x, y, z = self.steps[n]
        return (x if self.folded else x + 1) * 9 + (y + 1) * 3 + z + 1

    def peer(self, n):
        x, y, z = self.steps[n]
        i, j, k = (lax.axis_index(axis) for axis in AXES)
        there = (1 - i if x else i) if self.folded else i + x, j + y, k + z
        tests = []
        for axis, step, position in zip(AXES, self.steps[n], there):
            if step and not (self.folded and axis == "gx"):
                tests.append(jnp.logical_and(position >= 0, position < lax.axis_size(axis)))
        return there, functools.reduce(jnp.logical_and, tests) if tests else None


def guarded(inside, action):
    if inside is None:
        action()
    else:
        pl.when(inside)(action)


def clear(slots, inbox, landed):
    for n in range(len(slots)):
        inside = slots.peer(n)[1]
        if inside is not None:

            @pl.when(jnp.logical_not(inside))
            def _():
                for r in range(inbox.shape[0]):
                    inbox[r, n] = jnp.zeros(inbox.shape[2:], inbox.dtype)

    position = [lax.axis_index(axis) for axis in AXES]
    for q in range(27):
        tests = [jnp.full((), q == 13)]
        for i, axis, step in zip(position, AXES, (q // 9 - 1, q // 3 % 3 - 1, q % 3 - 1)):
            if step:
                tests.append(i == (0 if step < 0 else lax.axis_size(axis) - 1))

        @pl.when(functools.reduce(jnp.logical_or, tests))
        def _():
            landed[q] = jnp.zeros(landed.shape[1:], landed.dtype)


def enter(slots):
    barrier = pltpu.get_barrier_semaphore()
    for n in range(len(slots)):
        there, inside = slots.peer(n)
        guarded(inside, lambda: pl.semaphore_signal(barrier, inc=1, device_id=there, device_id_type=MESH))
    peers = 1
    for axis in AXES:
        i, n = lax.axis_index(axis), lax.axis_size(axis)
        peers = peers * (1 + jnp.where(i > 0, 1, 0) + jnp.where(i < n - 1, 1, 0))
    return barrier, peers - 1


def remote(source, target, send_sem, recv_sem, there):
    return pltpu.make_async_remote_copy(
        src_ref=source, dst_ref=target, send_sem=send_sem, recv_sem=recv_sem,
        device_id=there, device_id_type=MESH,
    )


def send(slots, outbox, inbox, send_sems, recv_sems, by_direction=False):
    for n in reversed(range(len(slots))):
        there, inside = slots.peer(n)
        far = slots.opposite(n)
        q = slots.direction(n) if by_direction else n
        into = 26 - q if by_direction else far
        copy = remote(outbox.at[q], inbox.at[into], send_sems.at[n], recv_sems.at[far], there)
        guarded(inside, copy.start)


def land(slots, numbers, outbox, inbox, send_sems, recv_sems, by_direction=False):
    for n in numbers:
        there, inside = slots.peer(n)
        q = slots.direction(n) if by_direction else n
        copy = remote(outbox.at[q], inbox.at[q], send_sems.at[n], recv_sems.at[n], there)

        def both():
            copy.wait_recv()
            copy.wait_send()

        guarded(inside, both)


def encode_nodes(kin_ref, node_w1, node_w2, center_of, square, wide):
    features = node_w1.shape[0]
    square[...] = jnp.zeros_like(square)
    wide[...] = jnp.zeros_like(wide)
    first = node_w1[...]
    square[0:features, :] = first
    square[16 : 16 + features, :] = first
    square[32 : 32 + features, :] = first - head(first)
    moves = kin_ref[3:, :]
    wide[0:features, :] = moves
    wide[16 : 16 + features, :] = moves - head(moves)
    wide[32 : 32 + features, :] = moves
    hidden = jnp.maximum(dot(square[...].T.astype(BF16), wide[...].astype(BF16)), 0.0).astype(BF16)
    second = dot_nt(center_of, node_w2[...]).astype(BF16)
    return normed(dot(second, hidden)).astype(BF16)


def fill_send_hot(slots, send_ref, send_hot):
    ghosts = send_ref.shape[0]
    particles = send_hot.shape[1]
    position = iota((ghosts, particles), 1)
    for n in range(len(slots)):
        x, y, z = slots.steps[n]
        q = slots.place(n) + (9 if slots.folded else 0)
        wanted = send_ref[:, q : q + 1]
        if slots.folded and x == 1:
            wanted = jnp.where(lax.axis_index("gx") == 0, wanted, send_ref[:, q - 18 : q - 17])
        send_hot[n * ghosts : (n + 1) * ghosts, :] = jnp.where(position == wanted, 1.0, 0.0).astype(BF16)


def prepare_indices(slots, index_ref, local_code, ghost_code, row_code, ghosts):
    pair_slots, particles = index_ref.shape
    lanes = row_code.shape[1]
    index = index_ref[...]
    ghost = index - particles
    half = 9 * ghosts
    if slots.folded:
        code = jnp.where(ghost < half, ghost + half, ghost - half) - half
    else:
        code = ghost - 3 * half // 2
    local_code[...] = index.astype(F32)
    ghost_code[...] = jnp.where(index < particles, 255, code).astype(F32)
    steps = iota((16, lanes), 0)
    for b in range(particles // 16):
        row_code[16 * b : 16 * (b + 1), :] = (steps + 16 * b).astype(F32).astype(BF16)
    shift = half if slots.folded else 3 * half // 2
    rows = iota((ghosts, lanes), 0)
    for n in range(len(slots)):
        start = particles + n * ghosts
        row_code[start : start + ghosts, :] = (rows + (slots.place(n) * ghosts - shift)).astype(F32).astype(BF16)


def fill_pair_hot(k, local_code, ghost_code, row_code, own, near, far, width):
    particles = near.shape[2]
    near_ghosts = near.shape[1] - width
    one = jnp.ones((16, particles), BF16)
    zero = jnp.zeros((16, particles), BF16)
    local = jnp.broadcast_to(local_code[pl.ds(k, 1), :], (16, particles)).astype(BF16)
    ghost = jnp.broadcast_to(ghost_code[pl.ds(k, 1), :], (16, particles)).astype(BF16)

    def block(row, code):
        return jnp.where(row_code[row : row + 16, :] == code, one, zero)

    for b in range(particles // 16):
        own[k, 16 * b : 16 * (b + 1), :] = block(16 * b, local)
    for b in range(near_ghosts // 16):
        start = width + 16 * b
        near[k, start : start + 16, :] = block(particles + 16 * b, ghost)
    for b in range(far.shape[1] // 16):
        far[k, 16 * b : 16 * (b + 1), :] = block(particles + near_ghosts + 16 * b, ghost)


def edge_features(off_ref, edge_w1, square, feature):
    pair_slots = off_ref.shape[1]
    width = edge_w1.shape[1]
    x, y, z = off_ref[0], off_ref[1], off_ref[2]
    terms = (x, y, z, x * x + y * y + z * z)
    rows = 4 * pair_slots
    for c, term in enumerate(terms):
        high = term.astype(BF16)
        low = (term - high.astype(F32)).astype(BF16)
        feature[c * pair_slots : (c + 1) * pair_slots, :] = high
        feature[rows + c * pair_slots : rows + (c + 1) * pair_slots, :] = low
        feature[2 * rows + c * pair_slots : 2 * rows + (c + 1) * pair_slots, :] = high
    first = edge_w1[...]
    square[0:4, :] = first
    square[4:8, :] = first
    square[8:12, :] = first - head(first)
    spread_row = iota((width, 3 * rows), 0)
    spread_lane = iota((width, 3 * rows), 1)
    spread = jnp.where(spread_lane // pair_slots == spread_row, 1.0, 0.0).astype(BF16)
    return dot(square[...].T.astype(BF16), spread)


def step_kernel(slots, *refs):
    operands, results, scratch = refs[:19], refs[19:21], refs[21:]
    (
        kin_ref, off_ref, index_ref, count_ref, send_ref, dir_ref, slot_ref, enc_node_w1, enc_node_w2,
        enc_edge_w1, enc_edge_w2, edge_w1, edge_w2, node_w1, node_w2, edge_gain, node_gain, dec_w1,
        dec_w2,
    ) = copies = scratch[:19]
    stayed_ref, arrived_ref = results
    (
        copy_sems, outbox, inbox, leaving, landed, send_sems, recv_sems, square, wide, feature, base,
        local_code, ghost_code, row_code, send_hot, own, near, far, hidden, partial, squares, own_left,
        near_left, far_left, received, first_t, second_c, node_t, node_c, gains, both, state, rows,
    ) = scratch[19:]
    width = enc_node_w2.shape[1]
    state_rows, particles = kin_ref.shape
    pair_slots = index_ref.shape[0]
    ghosts = send_ref.shape[0]
    rounds = edge_w1.shape[0]
    faces = slots.faces

    barrier, peers = enter(slots)
    fetches = [
        pltpu.make_async_copy(source, target, copy_sems.at[n])
        for n, (source, target) in enumerate(zip(operands, copies))
    ]
    urgent = [4, 0, 7, 8]
    for n in urgent + [n for n in range(19) if n not in urgent]:
        fetches[n].start()
    clear(slots, inbox, landed)

    diagonal = iota((width, width), 0) == iota((width, width), 1)
    unit = jnp.where(diagonal, 1.0, 0.0).astype(BF16)
    center_of = jnp.where(diagonal, 1.0 - 1.0 / width, -1.0 / width).astype(BF16)

    for n in urgent:
        fetches[n].wait()
    fill_send_hot(slots, send_ref, send_hot)
    latent = encode_nodes(kin_ref, enc_node_w1, enc_node_w2, center_of, square, wide)
    both[0:width, :] = latent
    outbox[0] = dot_nt(send_hot[...], latent).astype(BF16).reshape(outbox.shape[1:])
    pl.semaphore_wait(barrier, peers)

    def path(r):
        return outbox.at[r], inbox.at[r], send_sems.at[r], recv_sems.at[r]

    def turn_weights(r):
        first_t[r] = dot_nt(unit, edge_w1[r]).astype(BF16)
        second_c[r] = dot_nt(center_of, edge_w2[r]).astype(BF16)
        node_t[r] = dot_nt(unit, node_w1[r]).astype(BF16)
        node_c[r] = dot_nt(center_of, node_w2[r]).astype(BF16)

    def local_part(r):
        weights = first_t.at[r]
        now = both[0:width, :]
        received[...] = dot(weights[:, width : 2 * width], now)
        own_left[...] = dot(weights[:, 2 * width :], now).astype(BF16)
        near_left[:, 0:width] = weights[:, 0:width]

    for r in range(rounds):
        send(slots, *path(r))
        if r == 0:
            for n in range(19):
                if n not in urgent:
                    fetches[n].wait()
            base[...] = edge_features(off_ref, enc_edge_w1, square, feature).astype(BF16)
            enc_second = dot_nt(center_of, enc_edge_w2[...]).astype(BF16)
            prepare_indices(slots, index_ref, local_code, ghost_code, row_code, ghosts)
            slot_of = iota(base.shape, 1) % pair_slots

            def first_edge(k, carry):
                left = jnp.where(slot_of == k, base[...].astype(F32), 0.0).astype(BF16)
                hidden[k] = jnp.maximum(dot(left, feature[...]), 0.0).astype(BF16)
                return carry

            lax.fori_loop(0, pair_slots, first_edge, 0, unroll=pair_slots)

            def second_edge(k, carry):
                fresh = normed(dot(enc_second, hidden[k])).astype(BF16)
                near[k, 0:width, :] = fresh
                fill_pair_hot(k, local_code, ghost_code, row_code, own, near, far, width)
                return carry

            lax.fori_loop(0, pair_slots, second_edge, 0, unroll=pair_slots)
            turn_weights(0)
            square[0:rounds, :] = edge_gain[...]
            square[rounds : 2 * rounds, :] = node_gain[...]
            columns = square[...].T
            for g in range(2 * rounds):
                gains[g] = jnp.broadcast_to(columns[:, g : g + 1], (width, width))
        local_part(r)

        def local(k, carry):
            partial[k] = dot(own_left[...], own[k]) + received[...]
            return carry

        lax.fori_loop(0, pair_slots, local, 0, unroll=pair_slots)
        if r + 1 < rounds:
            turn_weights(r + 1)
        land(slots, range(faces), *path(r))
        near_left[:, width:] = dot_nt(
            first_t[r, :, 2 * width :], inbox[r, 0:faces].reshape(-1, width)
        ).astype(BF16)

        def early(k, carry):
            partial[k] = partial[k] + dot(near_left[...], near[k])
            return carry

        lax.fori_loop(0, pair_slots, early, 0, unroll=pair_slots)
        land(slots, range(faces, len(slots)), *path(r))
        far_left[...] = dot_nt(
            first_t[r, :, 2 * width :], inbox[r, faces:].reshape(-1, width)
        ).astype(BF16)
        edge_column = jnp.concatenate([gains[r]] * (particles // width), axis=1)
        node_column = jnp.concatenate([gains[rounds + r]] * (particles // width), axis=1)
        for k in range(pair_slots):
            hidden[k] = jnp.maximum(partial[k] + dot(far_left[...], far[k]), 0.0).astype(BF16)
        for k in range(pair_slots):
            center = dot(second_c[r], hidden[k])
            partial[k] = center
            scale = inverse_spread(jnp.sum(center * center, axis=0, keepdims=True), width)
            scale = jnp.where(k < count_ref[...], scale, 0.0)
            squares[k] = jnp.broadcast_to(scale, squares.shape[1:])
        for f in range(0, width, 8):
            total = partial[0, f : f + 8, :] * squares[0]
            for k in range(1, pair_slots):
                total = total + partial[k, f : f + 8, :] * squares[k]
            received[f : f + 8, :] = total
        both[width : 2 * width, :] = (received[...] * edge_column).astype(BF16)
        middle = jnp.maximum(dot(node_t[r], both[...]), 0.0).astype(BF16)
        update = normed(dot(node_c[r], middle)) * node_column
        latent = (both[0:width, :].astype(F32) + update).astype(BF16)
        both[0:width, :] = latent
        if r + 1 < rounds:
            outbox[r + 1] = dot_nt(send_hot[...], latent).astype(BF16).reshape(outbox.shape[1:])

    reading = dec_w2[...]
    wide[...] = jnp.zeros_like(wide)
    wide[0:3, 0:width] = reading
    wide[8:11, 0:width] = reading - head(reading)
    wide[16:19, 0:width] = reading - head(reading) - head(reading - head(reading))
    readout = wide[0:32, 0:width].astype(BF16)
    decoded = jnp.maximum(dot(dot_nt(unit, dec_w1[...]).astype(BF16), latent), 0.0).astype(BF16)
    parts = dot(readout, decoded)
    velocity = kin_ref[state_rows - 3 :, :] + (parts[0:3, :] + (parts[8:11, :] + parts[16:19, :]))
    state[...] = jnp.zeros_like(state)
    state[0:3, :] = kin_ref[0:3, :] + velocity
    state[3 : state_rows - 3, :] = kin_ref[6:, :]
    state[state_rows - 3 : state_rows, :] = velocity
    staying = dir_ref[...] == 13
    target = jnp.where(staying, -1, dir_ref[...] * MIG + slot_ref[...])
    picker = jnp.where(iota((rows.shape[0], particles), 0) == target, 1.0, 0.0).astype(BF16)
    whole = state[...]
    high = whole.astype(BF16)
    rest = whole - high.astype(F32)
    middle = rest.astype(BF16)
    low = (rest - middle.astype(F32)).astype(BF16)
    rows[:, 0 : state.shape[0]] = dot_nt(picker, high) + dot_nt(picker, middle) + dot_nt(picker, low)
    for q in range(27):
        leaving[q] = rows[MIG * q : MIG * (q + 1), :]
    migration = (leaving, landed, send_sems.at[rounds], recv_sems.at[rounds])
    send(slots, *migration, by_direction=True)
    stayed_ref[...] = jnp.where(staying, state[0:state_rows, :], 0.0)
    land(slots, range(len(slots)), *migration, by_direction=True)
    for q in range(27):
        rows[MIG * q : MIG * (q + 1), :] = landed[q]
    arrived_ref[...] = rows[...].T[0:state_rows, 0 : 27 * MIG]


def deliver(stayed_ref, arrived_ref, stayed_out, arrived_out, sems):
    copies = [
        pltpu.make_async_copy(stayed_ref, stayed_out, sems.at[0]),
        pltpu.make_async_copy(arrived_ref, arrived_out, sems.at[1]),
    ]
    for copy in copies:
        copy.start()
    for copy in copies:
        copy.wait()


def on_device(
    kinematics, pair_offsets, pair_index, neighbour_count, send_rows, migrate_dir, migrate_slot,
    enc_node_w1, enc_node_w2, enc_edge_w1, enc_edge_w2, edge_w1, edge_w2, node_w1, node_w2,
    edge_gain, node_gain, dec_w1, dec_w2,
):
    width = enc_node_w2.shape[1]
    pair_slots, particles = pair_index.shape
    ghosts = send_rows.shape[1]
    state_rows = kinematics.shape[0]
    rounds = edge_w1.shape[0]
    slots = Slots([lax.axis_size(axis) for axis in AXES])
    count = len(slots)
    near_rows = width + slots.faces * ghosts
    far_rows = (count - slots.faces) * ghosts
    operands = (
        kinematics, pair_offsets, pair_index, neighbour_count.reshape(1, particles), send_rows.T,
        migrate_dir.reshape(1, particles), migrate_slot.reshape(1, particles), enc_node_w1,
        enc_node_w2, enc_edge_w1, enc_edge_w2, edge_w1, edge_w2, node_w1, node_w2, edge_gain,
        node_gain, dec_w1, dec_w2,
    )
    vmem = pl.BlockSpec(memory_space=pltpu.VMEM)
    anywhere = pl.BlockSpec(memory_space=pl.ANY)
    shapes = [(state_rows, particles), (state_rows, 27 * MIG)]
    found = pl.pallas_call(
        functools.partial(step_kernel, slots),
        name="step",
        in_specs=[anywhere] * len(operands),
        out_specs=[vmem, vmem],
        out_shape=[pltpu.VMEM(shape, F32) for shape in shapes],
        scratch_shapes=[pltpu.VMEM(operand.shape, operand.dtype) for operand in operands]
        + [
            pltpu.SemaphoreType.DMA((len(operands),)),
            pltpu.VMEM((rounds, count, ghosts, width), BF16),
            pltpu.VMEM((rounds, count, ghosts, width), BF16),
            pltpu.VMEM((27, MIG, width), F32),
            pltpu.VMEM((27, MIG, width), F32),
            pltpu.SemaphoreType.DMA((rounds + 1, count)),
            pltpu.SemaphoreType.DMA((rounds + 1, count)),
            pltpu.VMEM((width, width), F32),
            pltpu.VMEM((width, particles), F32),
            pltpu.VMEM((12 * pair_slots, particles), BF16),
            pltpu.VMEM((width, 12 * pair_slots), BF16),
            pltpu.VMEM((pair_slots, particles), F32),
            pltpu.VMEM((pair_slots, particles), F32),
            pltpu.VMEM((particles + count * ghosts, particles), BF16),
            pltpu.VMEM((count * ghosts, particles), BF16),
            pltpu.VMEM((pair_slots, particles, particles), BF16),
            pltpu.VMEM((pair_slots, near_rows, particles), BF16),
            pltpu.VMEM((pair_slots, far_rows, particles), BF16),
            pltpu.VMEM((pair_slots, width, particles), BF16),
            pltpu.VMEM((pair_slots, width, particles), F32),
            pltpu.VMEM((pair_slots, 8, particles), F32),
            pltpu.VMEM((width, particles), BF16),
            pltpu.VMEM((width, near_rows), BF16),
            pltpu.VMEM((width, far_rows), BF16),
            pltpu.VMEM((width, particles), F32),
            pltpu.VMEM((rounds, width, 3 * width), BF16),
            pltpu.VMEM((rounds, width, width), BF16),
            pltpu.VMEM((rounds, width, 2 * width), BF16),
            pltpu.VMEM((rounds, width, width), BF16),
            pltpu.VMEM((2 * rounds, width, width), F32),
            pltpu.VMEM((2 * width, particles), BF16),
            pltpu.VMEM((32, particles), F32),
            pltpu.VMEM((width, width), F32),
        ],
        compiler_params=pltpu.CompilerParams(collective_id=0, has_side_effects=True),
    )(*operands)
    found = [pltpu.with_memory_space_constraint(x, pltpu.VMEM) for x in found]
    return tuple(
        pl.pallas_call(
            deliver,
            name="deliver",
            in_specs=[vmem] * 2,
            out_specs=[anywhere] * 2,
            out_shape=[jax.ShapeDtypeStruct(shape, F32) for shape in shapes],
            scratch_shapes=[pltpu.SemaphoreType.DMA((2,))],
            compiler_params=pltpu.CompilerParams(vmem_limit_bytes=1 << 20),
        )(*found)
    )


def solution(mesh):
    split = ("gx", "gy", "gz")
    return jax.shard_map(
        on_device,
        mesh=mesh,
        in_specs=(
            P(None, split),
            P(None, None, split),
            P(None, split),
            P(split),
            P(None, split),
            P(split),
            P(split),
        )
        + (P(),) * 12,
        out_specs=(P(None, split), P(None, split)),
        check_vma=False,
    )
```

```python
import functools

import jax
import jax.numpy as jnp
from jax import lax
from jax.experimental import pallas as pl
from jax.experimental.pallas import tpu as pltpu
from jax.sharding import PartitionSpec as P

MIG = 4

norm_eps = 1e-05
F32 = jnp.float32
BF16 = jnp.bfloat16
I32 = jnp.int32
MESH = pl.DeviceIdType.MESH
AXES = ("gx", "gy", "gz")


def dot(a, b):
    return jnp.dot(a, b, preferred_element_type=F32)


def dot_nt(a, b):
    return lax.dot_general(a, b, (((1,), (1,)), ((), ())), preferred_element_type=F32)


def iota(shape, axis):
    return lax.broadcasted_iota(I32, shape, axis)


def head(values):
    return values.astype(BF16).astype(F32)


def inverse_spread(square_sum, width):
    return lax.rsqrt(square_sum * (1.0 / width) + norm_eps)


def fold_rows(values):
    rows, lanes = values.shape
    return jnp.sum(values.reshape(rows // 8, 8, lanes), axis=0)


def normed(center):
    return center * inverse_spread(jnp.sum(center * center, axis=0, keepdims=True), center.shape[0])


class Slots:
    def __init__(self, sizes):
        self.folded = sizes[0] == 2
        steps = [(q // 9 - 1, q // 3 % 3 - 1, q % 3 - 1) for q in range(27) if q != 13]
        if self.folded:
            steps = [s for s in steps if s[0] >= 0]
        hops = lambda step: sum(map(abs, step))
        self.steps = sorted(steps, key=hops)
        self.faces = sum(hops(step) == 1 for step in steps)
        self.number = {s: n for n, s in enumerate(self.steps)}

    def __len__(self):
        return len(self.steps)

    def opposite(self, n):
        x, y, z = self.steps[n]
        return self.number[(x if self.folded else -x, -y, -z)]

    def direction(self, n):
        x, y, z = self.steps[n]
        rest = (y + 1) * 3 + z + 1
        if self.folded and x == 1:
            return rest + 18 - 18 * lax.axis_index("gx")
        return rest + (x + 1) * 9

    def place(self, n):
        x, y, z = self.steps[n]
        return (x if self.folded else x + 1) * 9 + (y + 1) * 3 + z + 1

    def peer(self, n):
        x, y, z = self.steps[n]
        i, j, k = (lax.axis_index(axis) for axis in AXES)
        there = (1 - i if x else i) if self.folded else i + x, j + y, k + z
        tests = []
        for axis, step, position in zip(AXES, self.steps[n], there):
            if step and not (self.folded and axis == "gx"):
                tests.append(jnp.logical_and(position >= 0, position < lax.axis_size(axis)))
        return there, functools.reduce(jnp.logical_and, tests) if tests else None


def guarded(inside, action):
    if inside is None:
        action()
    else:
        pl.when(inside)(action)


def clear(slots, inbox, landed):
    for n in range(len(slots)):
        inside = slots.peer(n)[1]
        if inside is not None:

            @pl.when(jnp.logical_not(inside))
            def _():
                for r in range(inbox.shape[0]):
                    inbox[r, n] = jnp.zeros(inbox.shape[2:], inbox.dtype)

    position = [lax.axis_index(axis) for axis in AXES]
    for q in range(27):
        tests = [jnp.full((), q == 13)]
        for i, axis, step in zip(position, AXES, (q // 9 - 1, q // 3 % 3 - 1, q % 3 - 1)):
            if step:
                tests.append(i == (0 if step < 0 else lax.axis_size(axis) - 1))

        @pl.when(functools.reduce(jnp.logical_or, tests))
        def _():
            landed[q] = jnp.zeros(landed.shape[1:], landed.dtype)


def enter(slots):
    barrier = pltpu.get_barrier_semaphore()
    for n in reversed(range(len(slots))):
        there, inside = slots.peer(n)
        guarded(inside, lambda: pl.semaphore_signal(barrier, inc=1, device_id=there, device_id_type=MESH))
    peers = 1
    for axis in AXES:
        i, n = lax.axis_index(axis), lax.axis_size(axis)
        peers = peers * (1 + jnp.where(i > 0, 1, 0) + jnp.where(i < n - 1, 1, 0))
    return barrier, peers - 1


def remote(source, target, send_sem, recv_sem, there):
    return pltpu.make_async_remote_copy(
        src_ref=source, dst_ref=target, send_sem=send_sem, recv_sem=recv_sem,
        device_id=there, device_id_type=MESH,
    )


def send(slots, outbox, inbox, send_sems, recv_sems, by_direction=False):
    for n in reversed(range(len(slots))):
        there, inside = slots.peer(n)
        far = slots.opposite(n)
        q = slots.direction(n) if by_direction else n
        into = 26 - q if by_direction else far
        copy = remote(outbox.at[q], inbox.at[into], send_sems.at[n], recv_sems.at[far], there)
        guarded(inside, copy.start)


def land(slots, numbers, outbox, inbox, send_sems, recv_sems, by_direction=False):
    for n in numbers:
        there, inside = slots.peer(n)
        q = slots.direction(n) if by_direction else n
        copy = remote(outbox.at[q], inbox.at[q], send_sems.at[n], recv_sems.at[n], there)

        def both():
            copy.wait_recv()
            copy.wait_send()

        guarded(inside, both)


def encode_nodes(kin_ref, node_w1, node_w2, center_of, square, wide):
    features = node_w1.shape[0]
    square[...] = jnp.zeros_like(square)
    wide[...] = jnp.zeros_like(wide)
    first = node_w1[...]
    square[0:features, :] = first
    square[16 : 16 + features, :] = first
    square[32 : 32 + features, :] = first - head(first)
    moves = kin_ref[3:, :]
    wide[0:features, :] = moves
    wide[16 : 16 + features, :] = moves - head(moves)
    wide[32 : 32 + features, :] = moves
    hidden = jnp.maximum(dot(square[...].T.astype(BF16), wide[...].astype(BF16)), 0.0).astype(BF16)
    second = dot_nt(center_of, node_w2[...]).astype(BF16)
    return normed(dot(second, hidden)).astype(BF16)


def fill_send_hot(slots, send_ref, send_hot):
    ghosts = send_ref.shape[0]
    particles = send_hot.shape[1]
    position = iota((ghosts, particles), 1)
    for n in range(len(slots)):
        x, y, z = slots.steps[n]
        q = slots.place(n) + (9 if slots.folded else 0)
        wanted = send_ref[:, q : q + 1]
        if slots.folded and x == 1:
            wanted = jnp.where(lax.axis_index("gx") == 0, wanted, send_ref[:, q - 18 : q - 17])
        send_hot[n * ghosts : (n + 1) * ghosts, :] = jnp.where(position == wanted, 1.0, 0.0).astype(BF16)


def prepare_indices(slots, index_ref, local_code, ghost_code, row_code, ghosts):
    pair_slots, particles = index_ref.shape
    lanes = row_code.shape[1]
    index = index_ref[...]
    ghost = index - particles
    half = 9 * ghosts
    if slots.folded:
        code = jnp.where(ghost < half, ghost + half, ghost - half) - half
    else:
        code = ghost - 3 * half // 2
    local_code[...] = index.astype(F32)
    ghost_code[...] = jnp.where(index < particles, 255, code).astype(F32)
    steps = iota((16, lanes), 0)
    for b in range(particles // 16):
        row_code[16 * b : 16 * (b + 1), :] = (steps + 16 * b).astype(F32).astype(BF16)
    shift = half if slots.folded else 3 * half // 2
    rows = iota((ghosts, lanes), 0)
    for n in range(len(slots)):
        start = particles + n * ghosts
        row_code[start : start + ghosts, :] = (rows + (slots.place(n) * ghosts - shift)).astype(F32).astype(BF16)


def fill_pair_hot(k, local_code, ghost_code, row_code, own, near, far, width):
    particles = near.shape[2]
    near_ghosts = near.shape[1] - width
    one = jnp.ones((16, particles), BF16)
    zero = jnp.zeros((16, particles), BF16)
    local = jnp.broadcast_to(local_code[pl.ds(k, 1), :], (16, particles)).astype(BF16)
    ghost = jnp.broadcast_to(ghost_code[pl.ds(k, 1), :], (16, particles)).astype(BF16)

    def block(row, code):
        return jnp.where(row_code[row : row + 16, :] == code, one, zero)

    for b in range(particles // 16):
        own[k, 16 * b : 16 * (b + 1), :] = block(16 * b, local)
    for b in range(near_ghosts // 16):
        start = width + 16 * b
        near[k, start : start + 16, :] = block(particles + 16 * b, ghost)
    for b in range(far.shape[1] // 16):
        far[k, 16 * b : 16 * (b + 1), :] = block(particles + near_ghosts + 16 * b, ghost)


def edge_features(off_ref, edge_w1, square, feature):
    pair_slots = off_ref.shape[1]
    width = edge_w1.shape[1]
    x, y, z = off_ref[0], off_ref[1], off_ref[2]
    terms = (x, y, z, x * x + y * y + z * z)
    rows = 4 * pair_slots
    for c, term in enumerate(terms):
        high = term.astype(BF16)
        low = (term - high.astype(F32)).astype(BF16)
        feature[c * pair_slots : (c + 1) * pair_slots, :] = high
        feature[rows + c * pair_slots : rows + (c + 1) * pair_slots, :] = low
        feature[2 * rows + c * pair_slots : 2 * rows + (c + 1) * pair_slots, :] = high
    first = edge_w1[...]
    square[0:4, :] = first
    square[4:8, :] = first
    square[8:12, :] = first - head(first)
    spread_row = iota((width, 3 * rows), 0)
    spread_lane = iota((width, 3 * rows), 1)
    spread = jnp.where(spread_lane // pair_slots == spread_row, 1.0, 0.0).astype(BF16)
    return dot(square[...].T.astype(BF16), spread)


def step_kernel(slots, *refs):
    operands, results, scratch = refs[:19], refs[19:21], refs[21:]
    (
        kin_ref, off_ref, index_ref, count_ref, send_ref, dir_ref, slot_ref, enc_node_w1, enc_node_w2,
        enc_edge_w1, enc_edge_w2, edge_w1, edge_w2, node_w1, node_w2, edge_gain, node_gain, dec_w1,
        dec_w2,
    ) = copies = scratch[:19]
    stayed_ref, arrived_ref = results
    (
        copy_sems, outbox, inbox, leaving, landed, send_sems, recv_sems, square, wide, feature, base,
        local_code, ghost_code, row_code, send_hot, own, near, far, hidden, partial, squares, own_left,
        near_left, far_left, received, first_t, second_c, node_t, node_c, gains, both, state, rows, dec_t,
        picker,
    ) = scratch[19:]
    width = enc_node_w2.shape[1]
    state_rows, particles = kin_ref.shape
    pair_slots = index_ref.shape[0]
    ghosts = send_ref.shape[0]
    rounds = edge_w1.shape[0]
    faces = slots.faces

    barrier, peers = enter(slots)
    fetches = [
        pltpu.make_async_copy(source, target, copy_sems.at[n])
        for n, (source, target) in enumerate(zip(operands, copies))
    ]
    urgent = [4, 0, 7, 8]
    for n in urgent + [n for n in range(19) if n not in urgent]:
        fetches[n].start()
    clear(slots, inbox, landed)

    diagonal = iota((width, width), 0) == iota((width, width), 1)
    unit = jnp.where(diagonal, 1.0, 0.0).astype(BF16)
    center_of = jnp.where(diagonal, 1.0 - 1.0 / width, -1.0 / width).astype(BF16)

    for n in urgent:
        fetches[n].wait()
    fill_send_hot(slots, send_ref, send_hot)
    latent = encode_nodes(kin_ref, enc_node_w1, enc_node_w2, center_of, square, wide)
    both[0:width, :] = latent
    outbox[0] = dot_nt(send_hot[...], latent).astype(BF16).reshape(outbox.shape[1:])
    pl.semaphore_wait(barrier, peers)

    def path(r):
        return outbox.at[r], inbox.at[r], send_sems.at[r], recv_sems.at[r]

    def turn_weights(r):
        first_t[r] = dot_nt(unit, edge_w1[r]).astype(BF16)
        second_c[r] = dot_nt(center_of, edge_w2[r]).astype(BF16)
        node_t[r] = dot_nt(unit, node_w1[r]).astype(BF16)
        node_c[r] = dot_nt(center_of, node_w2[r]).astype(BF16)

    def local_part(r):
        weights = first_t.at[r]
        now = both[0:width, :]
        received[...] = dot(weights[:, width : 2 * width], now)
        own_left[...] = dot(weights[:, 2 * width :], now).astype(BF16)
        near_left[:, 0:width] = weights[:, 0:width]

    for r in range(rounds):
        send(slots, *path(r))
        if r == 0:
            for n in range(19):
                if n not in urgent:
                    fetches[n].wait()
            base[...] = edge_features(off_ref, enc_edge_w1, square, feature).astype(BF16)
            enc_second = dot_nt(center_of, enc_edge_w2[...]).astype(BF16)
            prepare_indices(slots, index_ref, local_code, ghost_code, row_code, ghosts)
            slot_of = iota(base.shape, 1) % pair_slots

            def first_edge(k, carry):
                left = jnp.where(slot_of == k, base[...].astype(F32), 0.0).astype(BF16)
                hidden[k] = jnp.maximum(dot(left, feature[...]), 0.0).astype(BF16)
                return carry

            lax.fori_loop(0, pair_slots, first_edge, 0, unroll=pair_slots)

            def second_edge(k, carry):
                fresh = normed(dot(enc_second, hidden[k])).astype(BF16)
                near[k, 0:width, :] = fresh
                fill_pair_hot(k, local_code, ghost_code, row_code, own, near, far, width)
                return carry

            lax.fori_loop(0, pair_slots, second_edge, 0, unroll=pair_slots)
            turn_weights(0)
            square[0:rounds, :] = edge_gain[...]
            square[rounds : 2 * rounds, :] = node_gain[...]
            columns = square[...].T
            for g in range(2 * rounds):
                gains[g] = jnp.broadcast_to(columns[:, g : g + 1], (width, width))
        local_part(r)

        def local(k, carry):
            partial[k] = dot(own_left[...], own[k]) + received[...]
            return carry

        lax.fori_loop(0, pair_slots, local, 0, unroll=pair_slots)
        if r + 1 < rounds:
            turn_weights(r + 1)
        else:
            reading = dec_w2[...]
            wide[...] = jnp.zeros_like(wide)
            wide[0:3, 0:width] = reading
            wide[8:11, 0:width] = reading - head(reading)
            wide[16:19, 0:width] = reading - head(reading) - head(reading - head(reading))
            dec_t[...] = dot_nt(unit, dec_w1[...]).astype(BF16)
            target = jnp.where(dir_ref[...] == 13, -1, dir_ref[...] * MIG + slot_ref[...])
            picker[...] = jnp.where(iota(picker.shape, 0) == target, 1.0, 0.0).astype(BF16)
        land(slots, range(faces), *path(r))
        near_left[:, width:] = dot_nt(
            first_t[r, :, 2 * width :], inbox[r, 0:faces].reshape(-1, width)
        ).astype(BF16)

        def early(k, carry):
            partial[k] = partial[k] + dot(near_left[...], near[k])
            return carry

        lax.fori_loop(0, pair_slots, early, 0, unroll=pair_slots)
        land(slots, range(faces, len(slots)), *path(r))
        far_left[...] = dot_nt(
            first_t[r, :, 2 * width :], inbox[r, faces:].reshape(-1, width)
        ).astype(BF16)
        edge_column = jnp.concatenate([gains[r]] * (particles // width), axis=1)
        node_column = jnp.concatenate([gains[rounds + r]] * (particles // width), axis=1)
        for k in range(pair_slots):
            hidden[k] = jnp.maximum(partial[k] + dot(far_left[...], far[k]), 0.0).astype(BF16)
        for k in range(pair_slots):
            center = dot(second_c[r], hidden[k])
            partial[k] = center
            scale = inverse_spread(jnp.sum(center * center, axis=0, keepdims=True), width)
            scale = jnp.where(k < count_ref[...], scale, 0.0)
            squares[k] = jnp.broadcast_to(scale, squares.shape[1:])
        half = pair_slots // 2
        for start in (0, half):
            members = range(start, start + half)
            scales = [squares[k] for k in members]
            for f in range(0, width, 8):
                total = functools.reduce(
                    jnp.add, [partial[k, f : f + 8, :] * scale for k, scale in zip(members, scales)]
                )
                received[f : f + 8, :] = total + received[f : f + 8, :] if start else total
        both[width : 2 * width, :] = (received[...] * edge_column).astype(BF16)
        middle = jnp.maximum(dot(node_t[r], both[...]), 0.0).astype(BF16)
        update = normed(dot(node_c[r], middle)) * node_column
        latent = (both[0:width, :].astype(F32) + update).astype(BF16)
        both[0:width, :] = latent
        if r + 1 < rounds:
            outbox[r + 1] = dot_nt(send_hot[...], latent).astype(BF16).reshape(outbox.shape[1:])

    decoded = jnp.maximum(dot(dec_t[...], latent), 0.0).astype(BF16)
    parts = dot(wide[0:32, 0:width].astype(BF16), decoded)
    velocity = kin_ref[state_rows - 3 :, :] + (parts[0:3, :] + (parts[8:11, :] + parts[16:19, :]))
    state[...] = jnp.zeros_like(state)
    state[0:3, :] = kin_ref[0:3, :] + velocity
    state[3 : state_rows - 3, :] = kin_ref[6:, :]
    state[state_rows - 3 : state_rows, :] = velocity
    staying = dir_ref[...] == 13
    whole = state[...]
    high = whole.astype(BF16)
    rest = whole - high.astype(F32)
    middle = rest.astype(BF16)
    low = (rest - middle.astype(F32)).astype(BF16)
    rows[:, 0 : state.shape[0]] = (
        dot_nt(picker[...], high) + dot_nt(picker[...], middle) + dot_nt(picker[...], low)
    )
    for q in range(27):
        leaving[q] = rows[MIG * q : MIG * (q + 1), :]
    migration = (leaving, landed, send_sems.at[rounds], recv_sems.at[rounds])
    send(slots, *migration, by_direction=True)
    stayed_ref[...] = jnp.where(staying, state[0:state_rows, :], 0.0)
    land(slots, range(len(slots)), *migration, by_direction=True)
    for q in range(27):
        rows[MIG * q : MIG * (q + 1), :] = landed[q]
    arrived_ref[...] = rows[...].T[0:state_rows, 0 : 27 * MIG]


def deliver(stayed_ref, arrived_ref, stayed_out, arrived_out, sems):
    copies = [
        pltpu.make_async_copy(stayed_ref, stayed_out, sems.at[0]),
        pltpu.make_async_copy(arrived_ref, arrived_out, sems.at[1]),
    ]
    for copy in copies:
        copy.start()
    for copy in copies:
        copy.wait()


def on_device(
    kinematics, pair_offsets, pair_index, neighbour_count, send_rows, migrate_dir, migrate_slot,
    enc_node_w1, enc_node_w2, enc_edge_w1, enc_edge_w2, edge_w1, edge_w2, node_w1, node_w2,
    edge_gain, node_gain, dec_w1, dec_w2,
):
    width = enc_node_w2.shape[1]
    pair_slots, particles = pair_index.shape
    ghosts = send_rows.shape[1]
    state_rows = kinematics.shape[0]
    rounds = edge_w1.shape[0]
    slots = Slots([lax.axis_size(axis) for axis in AXES])
    count = len(slots)
    near_rows = width + slots.faces * ghosts
    far_rows = (count - slots.faces) * ghosts
    operands = (
        kinematics, pair_offsets, pair_index, neighbour_count.reshape(1, particles), send_rows.T,
        migrate_dir.reshape(1, particles), migrate_slot.reshape(1, particles), enc_node_w1,
        enc_node_w2, enc_edge_w1, enc_edge_w2, edge_w1, edge_w2, node_w1, node_w2, edge_gain,
        node_gain, dec_w1, dec_w2,
    )
    vmem = pl.BlockSpec(memory_space=pltpu.VMEM)
    anywhere = pl.BlockSpec(memory_space=pl.ANY)
    shapes = [(state_rows, particles), (state_rows, 27 * MIG)]
    found = pl.pallas_call(
        functools.partial(step_kernel, slots),
        name="step",
        in_specs=[anywhere] * len(operands),
        out_specs=[vmem, vmem],
        out_shape=[pltpu.VMEM(shape, F32) for shape in shapes],
        scratch_shapes=[pltpu.VMEM(operand.shape, operand.dtype) for operand in operands]
        + [
            pltpu.SemaphoreType.DMA((len(operands),)),
            pltpu.VMEM((rounds, count, ghosts, width), BF16),
            pltpu.VMEM((rounds, count, ghosts, width), BF16),
            pltpu.VMEM((27, MIG, width), F32),
            pltpu.VMEM((27, MIG, width), F32),
            pltpu.SemaphoreType.DMA((rounds + 1, count)),
            pltpu.SemaphoreType.DMA((rounds + 1, count)),
            pltpu.VMEM((width, width), F32),
            pltpu.VMEM((width, particles), F32),
            pltpu.VMEM((12 * pair_slots, particles), BF16),
            pltpu.VMEM((width, 12 * pair_slots), BF16),
            pltpu.VMEM((pair_slots, particles), F32),
            pltpu.VMEM((pair_slots, particles), F32),
            pltpu.VMEM((particles + count * ghosts, particles), BF16),
            pltpu.VMEM((count * ghosts, particles), BF16),
            pltpu.VMEM((pair_slots, particles, particles), BF16),
            pltpu.VMEM((pair_slots, near_rows, particles), BF16),
            pltpu.VMEM((pair_slots, far_rows, particles), BF16),
            pltpu.VMEM((pair_slots, width, particles), BF16),
            pltpu.VMEM((pair_slots, width, particles), F32),
            pltpu.VMEM((pair_slots, 8, particles), F32),
            pltpu.VMEM((width, particles), BF16),
            pltpu.VMEM((width, near_rows), BF16),
            pltpu.VMEM((width, far_rows), BF16),
            pltpu.VMEM((width, particles), F32),
            pltpu.VMEM((rounds, width, 3 * width), BF16),
            pltpu.VMEM((rounds, width, width), BF16),
            pltpu.VMEM((rounds, width, 2 * width), BF16),
            pltpu.VMEM((rounds, width, width), BF16),
            pltpu.VMEM((2 * rounds, width, width), F32),
            pltpu.VMEM((2 * width, particles), BF16),
            pltpu.VMEM((32, particles), F32),
            pltpu.VMEM((width, width), F32),
            pltpu.VMEM((width, width), BF16),
            pltpu.VMEM((width, particles), BF16),
        ],
        compiler_params=pltpu.CompilerParams(collective_id=0, has_side_effects=True),
    )(*operands)
    found = [pltpu.with_memory_space_constraint(x, pltpu.VMEM) for x in found]
    return tuple(
        pl.pallas_call(
            deliver,
            name="deliver",
            in_specs=[vmem] * 2,
            out_specs=[anywhere] * 2,
            out_shape=[jax.ShapeDtypeStruct(shape, F32) for shape in shapes],
            scratch_shapes=[pltpu.SemaphoreType.DMA((2,))],
            compiler_params=pltpu.CompilerParams(vmem_limit_bytes=1 << 20),
        )(*found)
    )


def solution(mesh):
    split = ("gx", "gy", "gz")
    return jax.shard_map(
        on_device,
        mesh=mesh,
        in_specs=(
            P(None, split),
            P(None, None, split),
            P(None, split),
            P(split),
            P(None, split),
            P(split),
            P(split),
        )
        + (P(),) * 12,
        out_specs=(P(None, split), P(None, split)),
        check_vma=False,
    )
```

```python
import functools

import jax
import jax.numpy as jnp
from jax import lax
from jax.experimental import pallas as pl
from jax.experimental.pallas import tpu as pltpu
from jax.sharding import PartitionSpec as P

MIG = 4

norm_eps = 1e-05
F32 = jnp.float32
BF16 = jnp.bfloat16
I32 = jnp.int32
MESH = pl.DeviceIdType.MESH
AXES = ("gx", "gy", "gz")


def dot(a, b):
    return jnp.dot(a, b, preferred_element_type=F32)


def dot_nt(a, b):
    return lax.dot_general(a, b, (((1,), (1,)), ((), ())), preferred_element_type=F32)


def iota(shape, axis):
    return lax.broadcasted_iota(I32, shape, axis)


def head(values):
    return values.astype(BF16).astype(F32)


def inverse_spread(square_sum, width):
    return lax.rsqrt(square_sum * (1.0 / width) + norm_eps)


def fold_rows(values):
    rows, lanes = values.shape
    return jnp.sum(values.reshape(rows // 8, 8, lanes), axis=0)


def normed(center):
    return center * inverse_spread(jnp.sum(center * center, axis=0, keepdims=True), center.shape[0])


class Slots:
    def __init__(self, sizes):
        self.folded = sizes[0] == 2
        steps = [(q // 9 - 1, q // 3 % 3 - 1, q % 3 - 1) for q in range(27) if q != 13]
        if self.folded:
            steps = [s for s in steps if s[0] >= 0]
        hops = lambda step: sum(map(abs, step))
        self.steps = sorted(steps, key=hops)
        self.faces = sum(hops(step) == 1 for step in steps)
        self.number = {s: n for n, s in enumerate(self.steps)}

    def __len__(self):
        return len(self.steps)

    def opposite(self, n):
        x, y, z = self.steps[n]
        return self.number[(x if self.folded else -x, -y, -z)]

    def direction(self, n):
        x, y, z = self.steps[n]
        rest = (y + 1) * 3 + z + 1
        if self.folded and x == 1:
            return rest + 18 - 18 * lax.axis_index("gx")
        return rest + (x + 1) * 9

    def place(self, n):
        x, y, z = self.steps[n]
        return (x if self.folded else x + 1) * 9 + (y + 1) * 3 + z + 1

    def peer(self, n):
        x, y, z = self.steps[n]
        i, j, k = (lax.axis_index(axis) for axis in AXES)
        there = (1 - i if x else i) if self.folded else i + x, j + y, k + z
        tests = []
        for axis, step, position in zip(AXES, self.steps[n], there):
            if step and not (self.folded and axis == "gx"):
                tests.append(jnp.logical_and(position >= 0, position < lax.axis_size(axis)))
        return there, functools.reduce(jnp.logical_and, tests) if tests else None


def guarded(inside, action):
    if inside is None:
        action()
    else:
        pl.when(inside)(action)


def clear(slots, inbox, landed):
    for n in range(len(slots)):
        inside = slots.peer(n)[1]
        if inside is not None:

            @pl.when(jnp.logical_not(inside))
            def _():
                for r in range(inbox.shape[0]):
                    inbox[r, n] = jnp.zeros(inbox.shape[2:], inbox.dtype)

    position = [lax.axis_index(axis) for axis in AXES]
    for q in range(27):
        tests = [jnp.full((), q == 13)]
        for i, axis, step in zip(position, AXES, (q // 9 - 1, q // 3 % 3 - 1, q % 3 - 1)):
            if step:
                tests.append(i == (0 if step < 0 else lax.axis_size(axis) - 1))

        @pl.when(functools.reduce(jnp.logical_or, tests))
        def _():
            landed[q] = jnp.zeros(landed.shape[1:], landed.dtype)


def enter(slots):
    barrier = pltpu.get_barrier_semaphore()
    for n in reversed(range(len(slots))):
        there, inside = slots.peer(n)
        guarded(inside, lambda: pl.semaphore_signal(barrier, inc=1, device_id=there, device_id_type=MESH))
    peers = 1
    for axis in AXES:
        i, n = lax.axis_index(axis), lax.axis_size(axis)
        peers = peers * (1 + jnp.where(i > 0, 1, 0) + jnp.where(i < n - 1, 1, 0))
    return barrier, peers - 1


def remote(source, target, send_sem, recv_sem, there):
    return pltpu.make_async_remote_copy(
        src_ref=source, dst_ref=target, send_sem=send_sem, recv_sem=recv_sem,
        device_id=there, device_id_type=MESH,
    )


def send(slots, outbox, inbox, send_sems, recv_sems, by_direction=False):
    for n in reversed(range(len(slots))):
        there, inside = slots.peer(n)
        far = slots.opposite(n)
        q = slots.direction(n) if by_direction else n
        into = 26 - q if by_direction else far
        copy = remote(outbox.at[q], inbox.at[into], send_sems.at[n], recv_sems.at[far], there)
        guarded(inside, copy.start)


def land(slots, numbers, outbox, inbox, send_sems, recv_sems, by_direction=False):
    for n in numbers:
        there, inside = slots.peer(n)
        q = slots.direction(n) if by_direction else n
        copy = remote(outbox.at[q], inbox.at[q], send_sems.at[n], recv_sems.at[n], there)

        def both():
            copy.wait_recv()
            copy.wait_send()

        guarded(inside, both)


def encode_nodes(kin_ref, node_w1, node_w2, center_of, square, wide):
    features = node_w1.shape[0]
    square[...] = jnp.zeros_like(square)
    wide[...] = jnp.zeros_like(wide)
    first = node_w1[...]
    square[0:features, :] = first
    square[16 : 16 + features, :] = first
    square[32 : 32 + features, :] = first - head(first)
    moves = kin_ref[3:, :]
    wide[0:features, :] = moves
    wide[16 : 16 + features, :] = moves - head(moves)
    wide[32 : 32 + features, :] = moves
    hidden = jnp.maximum(dot(square[...].T.astype(BF16), wide[...].astype(BF16)), 0.0).astype(BF16)
    second = dot_nt(center_of, node_w2[...]).astype(BF16)
    return normed(dot(second, hidden)).astype(BF16)


def fill_send_hot(slots, send_ref, send_hot):
    ghosts = send_ref.shape[0]
    particles = send_hot.shape[1]
    position = iota((ghosts, particles), 1)
    for n in range(len(slots)):
        x, y, z = slots.steps[n]
        q = slots.place(n) + (9 if slots.folded else 0)
        wanted = send_ref[:, q : q + 1]
        if slots.folded and x == 1:
            wanted = jnp.where(lax.axis_index("gx") == 0, wanted, send_ref[:, q - 18 : q - 17])
        send_hot[n * ghosts : (n + 1) * ghosts, :] = jnp.where(position == wanted, 1.0, 0.0).astype(BF16)


def prepare_indices(slots, index_ref, local_code, ghost_code, row_code, ghosts):
    pair_slots, particles = index_ref.shape
    lanes = row_code.shape[1]
    index = index_ref[...]
    ghost = index - particles
    half = 9 * ghosts
    if slots.folded:
        code = jnp.where(ghost < half, ghost + half, ghost - half) - half
    else:
        code = ghost - 3 * half // 2
    local_code[...] = index.astype(F32)
    ghost_code[...] = jnp.where(index < particles, 255, code).astype(F32)
    steps = iota((16, lanes), 0)
    for b in range(particles // 16):
        row_code[16 * b : 16 * (b + 1), :] = (steps + 16 * b).astype(F32).astype(BF16)
    shift = half if slots.folded else 3 * half // 2
    rows = iota((ghosts, lanes), 0)
    for n in range(len(slots)):
        start = particles + n * ghosts
        row_code[start : start + ghosts, :] = (rows + (slots.place(n) * ghosts - shift)).astype(F32).astype(BF16)


def fill_pair_hot(k, local_code, ghost_code, row_code, own, near, far, width):
    particles = near.shape[2]
    near_ghosts = near.shape[1] - width
    one = jnp.ones((16, particles), BF16)
    zero = jnp.zeros((16, particles), BF16)
    local = jnp.broadcast_to(local_code[pl.ds(k, 1), :], (16, particles)).astype(BF16)
    ghost = jnp.broadcast_to(ghost_code[pl.ds(k, 1), :], (16, particles)).astype(BF16)

    def block(row, code):
        return jnp.where(row_code[row : row + 16, :] == code, one, zero)

    for b in range(particles // 16):
        own[k, 16 * b : 16 * (b + 1), :] = block(16 * b, local)
    for b in range(near_ghosts // 16):
        start = width + 16 * b
        near[k, start : start + 16, :] = block(particles + 16 * b, ghost)
    for b in range(far.shape[1] // 16):
        far[k, 16 * b : 16 * (b + 1), :] = block(particles + near_ghosts + 16 * b, ghost)


def edge_features(off_ref, edge_w1, square, feature):
    pair_slots = off_ref.shape[1]
    width = edge_w1.shape[1]
    x, y, z = off_ref[0], off_ref[1], off_ref[2]
    terms = (x, y, z, x * x + y * y + z * z)
    rows = 4 * pair_slots
    for c, term in enumerate(terms):
        high = term.astype(BF16)
        low = (term - high.astype(F32)).astype(BF16)
        feature[c * pair_slots : (c + 1) * pair_slots, :] = high
        feature[rows + c * pair_slots : rows + (c + 1) * pair_slots, :] = low
        feature[2 * rows + c * pair_slots : 2 * rows + (c + 1) * pair_slots, :] = high
    first = edge_w1[...]
    square[0:4, :] = first
    square[4:8, :] = first
    square[8:12, :] = first - head(first)
    spread_row = iota((width, 3 * rows), 0)
    spread_lane = iota((width, 3 * rows), 1)
    spread = jnp.where(spread_lane // pair_slots == spread_row, 1.0, 0.0).astype(BF16)
    return dot(square[...].T.astype(BF16), spread)


def step_kernel(slots, *refs):
    operands, results, scratch = refs[:19], refs[19:21], refs[21:]
    (
        kin_ref, off_ref, index_ref, count_ref, send_ref, dir_ref, slot_ref, enc_node_w1, enc_node_w2,
        enc_edge_w1, enc_edge_w2, edge_w1, edge_w2, node_w1, node_w2, edge_gain, node_gain, dec_w1,
        dec_w2,
    ) = copies = scratch[:19]
    stayed_ref, arrived_ref = results
    (
        copy_sems, outbox, inbox, leaving, landed, send_sems, recv_sems, square, wide, feature, base,
        local_code, ghost_code, row_code, send_hot, own, near, far, hidden, partial, squares, own_left,
        near_left, far_left, received, first_t, second_c, node_t, node_c, gains, both, state, rows, dec_t,
        picker, node_pre,
    ) = scratch[19:]
    width = enc_node_w2.shape[1]
    state_rows, particles = kin_ref.shape
    pair_slots = index_ref.shape[0]
    ghosts = send_ref.shape[0]
    rounds = edge_w1.shape[0]
    faces = slots.faces

    barrier, peers = enter(slots)
    fetches = [
        pltpu.make_async_copy(source, target, copy_sems.at[n])
        for n, (source, target) in enumerate(zip(operands, copies))
    ]
    urgent = [4, 0, 7, 8]
    for n in urgent + [n for n in range(19) if n not in urgent]:
        fetches[n].start()
    clear(slots, inbox, landed)

    diagonal = iota((width, width), 0) == iota((width, width), 1)
    unit = jnp.where(diagonal, 1.0, 0.0).astype(BF16)
    center_of = jnp.where(diagonal, 1.0 - 1.0 / width, -1.0 / width).astype(BF16)

    for n in urgent:
        fetches[n].wait()
    fill_send_hot(slots, send_ref, send_hot)
    latent = encode_nodes(kin_ref, enc_node_w1, enc_node_w2, center_of, square, wide)
    both[0:width, :] = latent
    outbox[0] = dot_nt(send_hot[...], latent).astype(BF16).reshape(outbox.shape[1:])
    pl.semaphore_wait(barrier, peers)

    def path(r):
        return outbox.at[r], inbox.at[r], send_sems.at[r], recv_sems.at[r]

    def turn_weights(r):
        first_t[r] = dot_nt(unit, edge_w1[r]).astype(BF16)
        second_c[r] = dot_nt(center_of, edge_w2[r]).astype(BF16)
        node_t[r] = dot_nt(unit, node_w1[r]).astype(BF16)
        node_c[r] = dot_nt(center_of, node_w2[r]).astype(BF16)

    def local_part(r):
        weights = first_t.at[r]
        now = both[0:width, :]
        received[...] = dot(weights[:, width : 2 * width], now)
        own_left[...] = dot(weights[:, 2 * width :], now).astype(BF16)
        near_left[:, 0:width] = weights[:, 0:width]

    for r in range(rounds):
        send(slots, *path(r))
        if r == 0:
            for n in range(19):
                if n not in urgent:
                    fetches[n].wait()
            base[...] = edge_features(off_ref, enc_edge_w1, square, feature).astype(BF16)
            enc_second = dot_nt(center_of, enc_edge_w2[...]).astype(BF16)
            prepare_indices(slots, index_ref, local_code, ghost_code, row_code, ghosts)
            slot_of = iota(base.shape, 1) % pair_slots

            def first_edge(k, carry):
                left = jnp.where(slot_of == k, base[...].astype(F32), 0.0).astype(BF16)
                hidden[k] = jnp.maximum(dot(left, feature[...]), 0.0).astype(BF16)
                return carry

            lax.fori_loop(0, pair_slots, first_edge, 0, unroll=pair_slots)

            def second_edge(k, carry):
                fresh = normed(dot(enc_second, hidden[k])).astype(BF16)
                near[k, 0:width, :] = fresh
                fill_pair_hot(k, local_code, ghost_code, row_code, own, near, far, width)
                return carry

            lax.fori_loop(0, pair_slots, second_edge, 0, unroll=pair_slots)
            turn_weights(0)
            square[0:rounds, :] = edge_gain[...]
            square[rounds : 2 * rounds, :] = node_gain[...]
            columns = square[...].T
            for g in range(2 * rounds):
                gains[g] = jnp.broadcast_to(columns[:, g : g + 1], (width, width))
        local_part(r)

        def local(k, carry):
            partial[k] = dot(own_left[...], own[k]) + received[...]
            return carry

        lax.fori_loop(0, pair_slots, local, 0, unroll=pair_slots)
        node_pre[...] = dot(node_t[r, :, 0:width], both[0:width, :])
        if r + 1 < rounds:
            turn_weights(r + 1)
        else:
            reading = dec_w2[...]
            wide[...] = jnp.zeros_like(wide)
            wide[0:3, 0:width] = reading
            wide[8:11, 0:width] = reading - head(reading)
            wide[16:19, 0:width] = reading - head(reading) - head(reading - head(reading))
            dec_t[...] = dot_nt(unit, dec_w1[...]).astype(BF16)
            target = jnp.where(dir_ref[...] == 13, -1, dir_ref[...] * MIG + slot_ref[...])
            picker[...] = jnp.where(iota(picker.shape, 0) == target, 1.0, 0.0).astype(BF16)
        land(slots, range(faces), *path(r))
        near_left[:, width:] = dot_nt(
            first_t[r, :, 2 * width :], inbox[r, 0:faces].reshape(-1, width)
        ).astype(BF16)

        def early(k, carry):
            partial[k] = partial[k] + dot(near_left[...], near[k])
            return carry

        lax.fori_loop(0, pair_slots, early, 0, unroll=pair_slots)
        land(slots, range(faces, len(slots)), *path(r))
        far_left[...] = dot_nt(
            first_t[r, :, 2 * width :], inbox[r, faces:].reshape(-1, width)
        ).astype(BF16)
        edge_column = jnp.concatenate([gains[r]] * (particles // width), axis=1)
        node_column = jnp.concatenate([gains[rounds + r]] * (particles // width), axis=1)
        for k in range(pair_slots):
            hidden[k] = jnp.maximum(partial[k] + dot(far_left[...], far[k]), 0.0).astype(BF16)
        for k in range(pair_slots):
            center = dot(second_c[r], hidden[k])
            partial[k] = center
            scale = inverse_spread(jnp.sum(center * center, axis=0, keepdims=True), width)
            scale = jnp.where(k < count_ref[...], scale, 0.0)
            squares[k] = jnp.broadcast_to(scale, squares.shape[1:])
        half = pair_slots // 2
        for start in (0, half):
            members = range(start, start + half)
            scales = [jnp.concatenate([squares[k]] * 2, axis=0) for k in members]
            for f in range(0, width, 16):
                total = functools.reduce(
                    jnp.add, [partial[k, f : f + 16, :] * scale for k, scale in zip(members, scales)]
                )
                if start:
                    total = (total + received[f : f + 16, :]) * edge_column[f : f + 16, :]
                    both[width + f : width + f + 16, :] = total.astype(BF16)
                else:
                    received[f : f + 16, :] = total
        added = dot(node_t[r, :, width:], both[width : 2 * width, :])
        middle = jnp.maximum(node_pre[...] + added, 0.0).astype(BF16)
        update = normed(dot(node_c[r], middle)) * node_column
        latent = (both[0:width, :].astype(F32) + update).astype(BF16)
        both[0:width, :] = latent
        if r + 1 < rounds:
            outbox[r + 1] = dot_nt(send_hot[...], latent).astype(BF16).reshape(outbox.shape[1:])

    decoded = jnp.maximum(dot(dec_t[...], latent), 0.0).astype(BF16)
    parts = dot(wide[0:32, 0:width].astype(BF16), decoded)
    velocity = kin_ref[state_rows - 3 :, :] + (parts[0:3, :] + (parts[8:11, :] + parts[16:19, :]))
    state[...] = jnp.zeros_like(state)
    state[0:3, :] = kin_ref[0:3, :] + velocity
    state[3 : state_rows - 3, :] = kin_ref[6:, :]
    state[state_rows - 3 : state_rows, :] = velocity
    staying = dir_ref[...] == 13
    whole = state[...]
    high = whole.astype(BF16)
    rest = whole - high.astype(F32)
    middle = rest.astype(BF16)
    low = (rest - middle.astype(F32)).astype(BF16)
    rows[:, 0 : state.shape[0]] = (
        dot_nt(picker[...], high) + dot_nt(picker[...], middle) + dot_nt(picker[...], low)
    )
    for q in range(27):
        leaving[q] = rows[MIG * q : MIG * (q + 1), :]
    migration = (leaving, landed, send_sems.at[rounds], recv_sems.at[rounds])
    send(slots, *migration, by_direction=True)
    stayed_ref[...] = jnp.where(staying, state[0:state_rows, :], 0.0)
    land(slots, range(len(slots)), *migration, by_direction=True)
    for q in range(27):
        rows[MIG * q : MIG * (q + 1), :] = landed[q]
    arrived_ref[...] = rows[...].T[0:state_rows, 0 : 27 * MIG]


def deliver(stayed_ref, arrived_ref, stayed_out, arrived_out, sems):
    copies = [
        pltpu.make_async_copy(stayed_ref, stayed_out, sems.at[0]),
        pltpu.make_async_copy(arrived_ref, arrived_out, sems.at[1]),
    ]
    for copy in copies:
        copy.start()
    for copy in copies:
        copy.wait()


def on_device(
    kinematics, pair_offsets, pair_index, neighbour_count, send_rows, migrate_dir, migrate_slot,
    enc_node_w1, enc_node_w2, enc_edge_w1, enc_edge_w2, edge_w1, edge_w2, node_w1, node_w2,
    edge_gain, node_gain, dec_w1, dec_w2,
):
    width = enc_node_w2.shape[1]
    pair_slots, particles = pair_index.shape
    ghosts = send_rows.shape[1]
    state_rows = kinematics.shape[0]
    rounds = edge_w1.shape[0]
    slots = Slots([lax.axis_size(axis) for axis in AXES])
    count = len(slots)
    near_rows = width + slots.faces * ghosts
    far_rows = (count - slots.faces) * ghosts
    operands = (
        kinematics, pair_offsets, pair_index, neighbour_count.reshape(1, particles), send_rows.T,
        migrate_dir.reshape(1, particles), migrate_slot.reshape(1, particles), enc_node_w1,
        enc_node_w2, enc_edge_w1, enc_edge_w2, edge_w1, edge_w2, node_w1, node_w2, edge_gain,
        node_gain, dec_w1, dec_w2,
    )
    vmem = pl.BlockSpec(memory_space=pltpu.VMEM)
    anywhere = pl.BlockSpec(memory_space=pl.ANY)
    shapes = [(state_rows, particles), (state_rows, 27 * MIG)]
    found = pl.pallas_call(
        functools.partial(step_kernel, slots),
        name="step",
        in_specs=[anywhere] * len(operands),
        out_specs=[vmem, vmem],
        out_shape=[pltpu.VMEM(shape, F32) for shape in shapes],
        scratch_shapes=[pltpu.VMEM(operand.shape, operand.dtype) for operand in operands]
        + [
            pltpu.SemaphoreType.DMA((len(operands),)),
            pltpu.VMEM((rounds, count, ghosts, width), BF16),
            pltpu.VMEM((rounds, count, ghosts, width), BF16),
            pltpu.VMEM((27, MIG, width), F32),
            pltpu.VMEM((27, MIG, width), F32),
            pltpu.SemaphoreType.DMA((rounds + 1, count)),
            pltpu.SemaphoreType.DMA((rounds + 1, count)),
            pltpu.VMEM((width, width), F32),
            pltpu.VMEM((width, particles), F32),
            pltpu.VMEM((12 * pair_slots, particles), BF16),
            pltpu.VMEM((width, 12 * pair_slots), BF16),
            pltpu.VMEM((pair_slots, particles), F32),
            pltpu.VMEM((pair_slots, particles), F32),
            pltpu.VMEM((particles + count * ghosts, particles), BF16),
            pltpu.VMEM((count * ghosts, particles), BF16),
            pltpu.VMEM((pair_slots, particles, particles), BF16),
            pltpu.VMEM((pair_slots, near_rows, particles), BF16),
            pltpu.VMEM((pair_slots, far_rows, particles), BF16),
            pltpu.VMEM((pair_slots, width, particles), BF16),
            pltpu.VMEM((pair_slots, width, particles), F32),
            pltpu.VMEM((pair_slots, 8, particles), F32),
            pltpu.VMEM((width, particles), BF16),
            pltpu.VMEM((width, near_rows), BF16),
            pltpu.VMEM((width, far_rows), BF16),
            pltpu.VMEM((width, particles), F32),
            pltpu.VMEM((rounds, width, 3 * width), BF16),
            pltpu.VMEM((rounds, width, width), BF16),
            pltpu.VMEM((rounds, width, 2 * width), BF16),
            pltpu.VMEM((rounds, width, width), BF16),
            pltpu.VMEM((2 * rounds, width, width), F32),
            pltpu.VMEM((2 * width, particles), BF16),
            pltpu.VMEM((32, particles), F32),
            pltpu.VMEM((width, width), F32),
            pltpu.VMEM((width, width), BF16),
            pltpu.VMEM((width, particles), BF16),
            pltpu.VMEM((width, particles), F32),
        ],
        compiler_params=pltpu.CompilerParams(
            collective_id=0, has_side_effects=True,
        ),
    )(*operands)
    found = [pltpu.with_memory_space_constraint(x, pltpu.VMEM) for x in found]
    return tuple(
        pl.pallas_call(
            deliver,
            name="deliver",
            in_specs=[vmem] * 2,
            out_specs=[anywhere] * 2,
            out_shape=[jax.ShapeDtypeStruct(shape, F32) for shape in shapes],
            scratch_shapes=[pltpu.SemaphoreType.DMA((2,))],
            compiler_params=pltpu.CompilerParams(vmem_limit_bytes=1 << 20),
        )(*found)
    )


def solution(mesh):
    split = ("gx", "gy", "gz")
    return jax.shard_map(
        on_device,
        mesh=mesh,
        in_specs=(
            P(None, split),
            P(None, None, split),
            P(None, split),
            P(split),
            P(None, split),
            P(split),
            P(split),
        )
        + (P(),) * 12,
        out_specs=(P(None, split), P(None, split)),
        check_vma=False,
    )
```
